32 devices in a mesh: gx: 8 (over z, core), gy: 4 (over y, x).
Axes of the slice: x: 2, y: 2, z: 4, core: 2. Of those that a mesh axis runs over, the one named last changes fastest.
Arguments:
- pressure: float32 [128, 64, 512], P('gx', 'gy'), may hold values from -6 to 6
- divergence: float32 [128, 64, 512], P('gx', 'gy'), may hold values from -8 to 8
- inverse_density: float32 [128, 64, 512], P('gx', 'gy'), may hold values from 0.2 to 5
Outputs:
- new_pressure: float32 [128, 64, 512], P('gx', 'gy')
The draws below stay inside these ranges and needn't reach their ends.
All inputs are finite; a program needn't handle non-finite values.
Results may differ from the reference program's by a relative error of at most 0.000021.
Values sent between devices are 32-bit elements; how exact they have to be, the bound alone decides.
No kernel may reach another device: no remote copies, remote signals or barrier semaphores. Data moves between devices by JAX's collectives and lax.ppermute only.
A program may use at most 320 MiB of HBM per device.

```python
import math
import jax
import jax.numpy as jnp

NZ = 512
CHEB = 2
COARSE = 4
NX = 128
NY = 64


def draw_divergence(key, part):
    rough = jax.random.normal(key, (NX, NY, NZ), jnp.float32)
    return jnp.clip(rough, -8.0, 8.0)


def levels(stream_key, extent, cuts, low, high):
    def one(axis_at, parts):
        heights = jax.random.uniform(jax.random.fold_in(jax.random.fold_in(stream_key, 6), axis_at), (parts,), jnp.float32, low / len(cuts), high / len(cuts))
        return jnp.repeat(jnp.exp(heights), extent[axis_at] // parts).reshape((-1,) + (1,) * (len(extent) - axis_at - 1))

    level = one(*cuts[0])
    for cut in cuts[1:]:
        level = level * one(*cut)
    return level


def normal_values(stream_key, shape, scale, most, pieces=(), kind=jnp.bfloat16):
    gain = levels(stream_key, shape, pieces, -0.22, 0.18) if pieces else 1.0
    drawn = jax.random.normal(stream_key, shape, jnp.float32) * scale * gain
    return jnp.minimum(jnp.maximum(drawn, -most), most).astype(kind)


def setup_inputs(seed: int = 0) -> dict:
    keys = jax.random.split(jax.random.key(seed), 4)
    return {
        "pressure": normal_values(keys[0], (NX, NY, NZ), 1.0, 6.0, ((0, 8), (1, 4)), jnp.float32),
        "divergence": draw_divergence(jax.random.fold_in(keys[3], 71), 0),
        "inverse_density": jnp.clip(jnp.exp(math.log(5.0) - 3.218876 * jax.random.uniform(keys[2], (NX, NY, NZ), jnp.float32) ** levels(keys[2], (NX, NY, NZ), ((0, 8), (1, 4)), -0.2, 0.2)), 0.2, 5.0),
    }


shift_fine = 0.05
bound_low = 0.3
bound_high = 2.0
jacobi_weight = 0.8
stencil_weights = (0.0, 0.5, 0.125, 0.0625)
weight_total = 5.0
face_offsets = [(1, 0, 0), (-1, 0, 0), (0, 1, 0), (0, -1, 0), (0, 0, 1), (0, 0, -1)]
neighbour_offsets = [(offset_x, offset_y, offset_z) for offset_x in (-1, 0, 1) for offset_y in (-1, 0, 1) for offset_z in (-1, 0, 1) if (offset_x, offset_y, offset_z) != (0, 0, 0)]


def neighbour(values, offsets):
    return jnp.roll(values, (-offsets[0], -offsets[1], -offsets[2]), (0, 1, 2))


def operate_seven(values, mobility, shift_value):
    summed = shift_value * values
    for offsets in face_offsets:
        summed = summed + 0.5 * (mobility + neighbour(mobility, offsets)) * (values - neighbour(values, offsets))
    return summed


def diag_seven(mobility, shift_value):
    summed = shift_value + jnp.zeros_like(mobility)
    for offsets in face_offsets:
        summed = summed + 0.5 * (mobility + neighbour(mobility, offsets))
    return summed


def operate_full(values, mobility, shift_value):
    summed = shift_value * values
    for offsets in neighbour_offsets:
        weight = stencil_weights[abs(offsets[0]) + abs(offsets[1]) + abs(offsets[2])]
        summed = summed + weight * 0.5 * (mobility + neighbour(mobility, offsets)) * (values - neighbour(values, offsets))
    return summed


def diag_full(mobility, shift_value):
    summed = shift_value + jnp.zeros_like(mobility)
    for offsets in neighbour_offsets:
        weight = stencil_weights[abs(offsets[0]) + abs(offsets[1]) + abs(offsets[2])]
        summed = summed + weight * 0.5 * (mobility + neighbour(mobility, offsets))
    return summed


def restrict(values):
    shape = values.shape
    return values.reshape(shape[0] // 2, 2, shape[1] // 2, 2, shape[2] // 2, 2).mean(axis=(1, 3, 5))


def prolong(values):
    return jnp.repeat(jnp.repeat(jnp.repeat(values, 2, 0), 2, 1), 2, 2)


def chebyshev(iterate, source, mobility, shift_value, zero_start, need_residual):
    midpoint = (bound_high + bound_low) / 2
    halfwidth = (bound_high - bound_low) / 2
    sigma_ratio = midpoint / halfwidth
    ratio_prev = 1.0 / sigma_ratio
    inverse = 1.0 / diag_seven(mobility, shift_value)
    if zero_start:
        residual = source
    else:
        residual = source - operate_seven(iterate, mobility, shift_value)
    update = inverse * residual / midpoint
    iterate = update if zero_start else iterate + update
    for repeat in range(1, CHEB):
        residual = residual - operate_seven(update, mobility, shift_value)
        ratio_next = 1.0 / (2.0 * sigma_ratio - ratio_prev)
        update = ratio_next * ratio_prev * update + (2.0 * ratio_next / halfwidth) * inverse * residual
        ratio_prev = ratio_next
        iterate = iterate + update
    if need_residual:
        residual = residual - operate_seven(update, mobility, shift_value)
    return iterate, residual


def reference(pressure, divergence, inverse_density):
    mob_fine = inverse_density
    fine, fine_res = chebyshev(pressure, divergence, mob_fine, shift_fine, False, True)
    mob_mid = restrict(mob_fine)
    source_mid = 4.0 * restrict(fine_res)
    middle_it, middle_res = chebyshev(source_mid, source_mid, mob_mid, 4.0 * shift_fine, True, True)
    mob_low = restrict(mob_mid)
    source_low = 4.0 * restrict(middle_res)
    coarse_shift = 16.0 * shift_fine
    weighted = jacobi_weight / diag_full(mob_low, coarse_shift)
    coarse = weighted * source_low
    for repeat in range(COARSE - 1):
        coarse = coarse + weighted * (source_low - operate_full(coarse, mob_low, coarse_shift))
    mean_src = jnp.mean(source_low)
    mean_cor = jnp.mean(coarse)
    mean_mob = jnp.mean(mob_low)
    coarse = coarse + jacobi_weight * (mean_src - coarse_shift * mean_cor) / (coarse_shift + weight_total * mean_mob)
    middle_it, unused = chebyshev(middle_it + prolong(coarse), source_mid, mob_mid, 4.0 * shift_fine, False, False)
    fine, unused = chebyshev(fine + prolong(middle_it), divergence, mob_fine, shift_fine, False, False)
    return fine
```

```python
import jax
import jax.numpy as jnp
from jax import lax
from jax.experimental import pallas as pl
from jax.experimental.pallas import tpu as pltpu
from jax.sharding import PartitionSpec as P

SWEEPS = 4
SHIFT = 0.05
CENTER = (2.0 + 0.3) / 2
HALF = (2.0 - 0.3) / 2
Q0 = CENTER / HALF
P0 = 1.0 / Q0
P1 = 1.0 / (2.0 * Q0 - P0)
ALPHA = P1 * P0
BETA = 2.0 * P1 / HALF
INV_C = 1.0 / CENTER
JACOBI = 0.8
WEIGHT_TOTAL = 5.0

FX = 3
FY = 4
MX = 4

F32 = jnp.float32
VMEM_LIMIT = 60 * 1024 * 1024


def nxt(v, axis):
    return pltpu.roll(v, v.shape[axis] - 1, axis)


def prv(v, axis):
    return pltpu.roll(v, 1, axis)


def coefficients(m_ref, kx, ky, kz, w_ref, rows, shift):
    def body(i, low):
        m = m_ref[i]
        fx = 0.5 * (m + m_ref[i + 1])
        fy = 0.5 * (m + nxt(m, 0))
        fz = 0.5 * (m + nxt(m, 1))
        kx[i] = fx
        ky[i] = fy
        kz[i] = fz
        w_ref[i] = 1.0 / (shift + (fx + low) + (fy + prv(fy, 0)) + (fz + prv(fz, 1)))
        return fx

    first = 0.5 * (m_ref[0] + m_ref[1])
    kx[0] = first
    lax.fori_loop(1, rows - 1, body, first)


def apply_row(v_ref, kx, ky, kz, i, shift):
    c = v_ref[i]
    acc = shift * c + kx[i] * (c - v_ref[i + 1]) + kx[i - 1] * (c - v_ref[i - 1])
    fy = ky[i] * (c - nxt(c, 0))
    fz = kz[i] * (c - nxt(c, 1))
    return acc + (fy - prv(fy, 0)) + (fz - prv(fz, 1)), c


def dot(a, b):
    return jnp.dot(a, b, precision=lax.Precision.HIGHEST, preferred_element_type=F32)


def pair_matrix(z, value):
    row = lax.broadcasted_iota(jnp.int32, (z, z // 2), 0)
    col = lax.broadcasted_iota(jnp.int32, (z, z // 2), 1)
    return jnp.where(row // 2 == col, value, 0.0).astype(F32)


def spread_matrix(z):
    row = lax.broadcasted_iota(jnp.int32, (z, 2 * z), 0)
    col = lax.broadcasted_iota(jnp.int32, (z, 2 * z), 1)
    return jnp.where(col // 2 == row, 1.0, 0.0).astype(F32)


LANES = 128


def put_lanes(tmp, a, val):
    for g in range(val.shape[1] // LANES):
        tmp[a, g] = val[:, g * LANES:(g + 1) * LANES]


def take_pairs(tmp, a, y0, ny, chunks):
    parts = [tmp[a, g, pl.ds(y0, ny, stride=2), :] + tmp[a, g, pl.ds(y0 + 1, ny, stride=2), :] for g in range(chunks)]
    return jnp.concatenate(parts, axis=1)


def repeat_rows(tmp, val):
    n, chunks = val.shape[0], val.shape[1] // LANES
    for g in range(chunks):
        part = val[:, g * LANES:(g + 1) * LANES]
        tmp[g, pl.ds(0, n, stride=2), :] = part
        tmp[g, pl.ds(1, n, stride=2), :] = part
    return jnp.concatenate([tmp[g] for g in range(chunks)], axis=1)


def halve(ref, tmp, x0, y0, nx, ny, value):
    z = ref.shape[2]
    for a in range(nx):
        put_lanes(tmp, a, ref[x0 + 2 * a] + ref[x0 + 2 * a + 1])
    s = jnp.concatenate([take_pairs(tmp, a, y0, ny, z // LANES) for a in range(nx)], axis=0)
    return dot(s, pair_matrix(z, value)).reshape(nx, ny, z // 2)


def pack_fine(x, b, m, *outs):
    X, Y = x.shape[0], x.shape[1]
    gxp, gxm, gyp, gym, cpp, cpm, cmp_, cmm = outs
    for out, sl in ((gxp, lambda k: slice(X - k, X)), (gxm, lambda k: slice(0, k))):
        out[0:3] = x[sl(3)]
        out[3:5] = b[sl(2)]
        out[5:8] = m[sl(3)]
    for out, sl in ((gyp, lambda k: slice(Y - k, Y)), (gym, lambda k: slice(0, k))):
        out[:, 0:3, :] = x[:, sl(3), :]
        out[:, 3:5, :] = b[:, sl(2), :]
        out[:, 5:8, :] = m[:, sl(3), :]
    for out, sx, sy in ((cpp, 1, 1), (cpm, 1, -1), (cmp_, -1, 1), (cmm, -1, -1)):
        rows = slice(X - 2, X) if sx > 0 else slice(0, 2)
        cols = slice(Y - 2, Y) if sy > 0 else slice(0, 2)
        out[:, 0:2, :] = x[rows, cols, :]
        out[:, 2:4, :] = b[rows, cols, :]
        out[:, 4:6, :] = m[rows, cols, :]
        out[:, 6:8, :] = m[rows, cols, :]


def smooth_fine(x, b, m, gxl, gxh, gyl, gyh, cll, clh, chl, chh,
                x1, r1, w, kx, ky, kz, b2, m2, sxp, sxm, syp, sym, spp, spm, smp, smm,
                xe, be, me, u, r, tmp):
    X, Y, Z = x.shape
    R = X + 2 * FX
    x_end, y_end = FX + X, FY + Y
    for ext, own, lo, n in ((xe, x, 0, 3), (be, b, 3, 2), (me, m, 5, 3)):
        ext[FX:x_end, FY:y_end, :] = own[...]
        ext[FX - n:FX, FY:y_end, :] = gxl[lo:lo + n]
        ext[x_end:x_end + n, FY:y_end, :] = gxh[lo:lo + n]
        ext[FX:x_end, FY - n:FY, :] = gyl[:, lo:lo + n, :]
        ext[FX:x_end, y_end:y_end + n, :] = gyh[:, lo:lo + n, :]
    for msg, rows, cols in ((cll, slice(FX - 2, FX), slice(FY - 2, FY)),
                            (clh, slice(FX - 2, FX), slice(y_end, y_end + 2)),
                            (chl, slice(x_end, x_end + 2), slice(FY - 2, FY)),
                            (chh, slice(x_end, x_end + 2), slice(y_end, y_end + 2))):
        xe[rows, cols, :] = msg[:, 0:2, :]
        be[rows, cols, :] = msg[:, 2:4, :]
        me[rows, cols, :] = msg[:, 4:6, :]
    coefficients(me, kx, ky, kz, w, R, SHIFT)

    def first(i, carry):
        ax, _ = apply_row(xe, kx, ky, kz, i, SHIFT)
        res = be[i] - ax
        r[i] = res
        u[i] = (w[i] * res) * INV_C
        return carry

    lax.fori_loop(1, R - 1, first, 0)

    def second(i, carry):
        au, c = apply_row(u, kx, ky, kz, i, SHIFT)
        res = r[i] - au
        r[i] = res
        up = ALPHA * c + BETA * (w[i] * res)
        xe[i] = xe[i] + c + up
        be[i] = up
        return carry

    lax.fori_loop(2, R - 2, second, 0)

    def third(i, carry):
        au, _ = apply_row(be, kx, ky, kz, i, SHIFT)
        r[i] = r[i] - au
        return carry

    lax.fori_loop(3, R - 3, third, 0)
    x1[...] = xe[FX:x_end, FY:y_end, :]
    r1[...] = r[FX:x_end, FY:y_end, :]
    nx, ny, nz = X // 2, Y // 2, Z // 2
    b2[...] = halve(r, tmp, FX, FY, nx, ny, 0.5)
    mm = halve(me, tmp, FX - 2, 0, nx + 2, ny + 4, 0.125)
    cells = mm[1:nx + 1, 2:2 + ny, :]
    m2[...] = cells
    fz = 0.5 * (cells + nxt(cells, 2))
    fzp = prv(fz, 2)
    diag = (4.0 * SHIFT + 0.5 * (4.0 * cells + mm[0:nx, 2:2 + ny, :] + mm[2:nx + 2, 2:2 + ny, :]
                                 + mm[1:nx + 1, 1:1 + ny, :] + mm[1:nx + 1, 3:3 + ny, :]) + (fz + fzp))
    u2 = (b2[...] * (1.0 / diag)) * INV_C
    bb = b2[...]
    sxp[0:1] = u2[nx - 4:nx - 3]
    sxp[1:4] = bb[nx - 3:nx]
    sxp[4:8] = cells[nx - 4:nx]
    sxm[0:3] = bb[0:3]
    sxm[3:4] = u2[3:4]
    sxm[4:8] = cells[0:4]
    syp[0:nx, 0:1, :] = u2[:, ny - 4:ny - 3, :]
    syp[0:nx, 1:4, :] = bb[:, ny - 3:ny, :]
    syp[0:nx, 4:8, :] = cells[:, ny - 4:ny, :]
    sym[0:nx, 0:3, :] = bb[:, 0:3, :]
    sym[0:nx, 3:4, :] = u2[:, 3:4, :]
    sym[0:nx, 4:8, :] = cells[:, 0:4, :]
    for dst, src in ((sxp, r1[X - 1]), (sxm, r1[0])):
        for h in range(2):
            for g in range(2):
                dst[8 + 2 * h + g] = src[h * ny:(h + 1) * ny, g * nz:(g + 1) * nz]
    for dst, j in ((syp, Y - 1), (sym, 0)):
        for h in range(2):
            for k in range(ny):
                row = r1[h * ny + k, j:j + 1, :]
                for g in range(2):
                    dst[nx + 2 * h + g, k:k + 1, :] = row[:, g * nz:(g + 1) * nz]
    for out, sx, sy in ((spp, 1, 1), (spm, 1, -1), (smp, -1, 1), (smm, -1, -1)):
        for k in range(4):
            i = nx - 4 + k if sx > 0 else k
            di = 4 - k if sx > 0 else k + 1
            for l in range(4):
                j = ny - 4 + l if sy > 0 else l
                dj = 4 - l if sy > 0 else l + 1
                val = u2 if di + dj == 5 else bb
                out[k, l:l + 1, :] = val[i, j:j + 1, :]
                out[k, 4 + l:5 + l, :] = cells[i, j:j + 1, :]


def smooth_mid(b2, m2, gxl, gxh, gyl, gyh, cll, clh, chl, chh,
               xm, rm, w, kx, ky, kz, out,
               qe, me, u, tmp):
    nx, ny, nz = b2.shape
    R = nx + 2 * MX
    shift = 4.0 * SHIFT
    xend, yend = MX + nx, MX + ny
    for ext, own, lo in ((qe, b2, 0), (me, m2, 4)):
        ext[MX:xend, MX:yend, :] = own[...]
        ext[0:MX, MX:yend, :] = gxl[lo:lo + 4]
        ext[xend:xend + MX, MX:yend, :] = gxh[lo:lo + 4]
        ext[MX:xend, 0:MX, :] = gyl[0:nx, lo:lo + 4, :]
        ext[MX:xend, yend:yend + MX, :] = gyh[0:nx, lo:lo + 4, :]
        for msg, rows, cols in ((cll, slice(0, MX), slice(0, MX)),
                                (clh, slice(0, MX), slice(yend, yend + MX)),
                                (chl, slice(xend, xend + MX), slice(0, MX)),
                                (chh, slice(xend, xend + MX), slice(yend, yend + MX))):
            ext[rows, cols, :] = msg[:, lo:lo + 4, :]
    coefficients(me, kx, ky, kz, w, R, shift)
    col = lax.broadcasted_iota(jnp.int32, (ny + 2 * MX, nz), 0)
    dcol = jnp.maximum(jnp.maximum(MX - col, col - (yend - 1)), 0)

    def first(i, carry):
        di = jnp.maximum(jnp.maximum(MX - i, i - (xend - 1)), 0)
        q = qe[i]
        sent = (dcol + di == 5) | (dcol == 4) | (di == 4)
        u[i] = jnp.where(sent, q, (w[i] * q) * INV_C)
        return carry

    u[0] = qe[0]
    u[R - 1] = qe[R - 1]
    lax.fori_loop(1, R - 1, first, 0)

    def second(i, carry):
        au, c = apply_row(u, kx, ky, kz, i, shift)
        res = qe[i] - au
        rm[i] = res
        up = ALPHA * c + BETA * (w[i] * res)
        xm[i] = c + up
        qe[i] = up
        return carry

    lax.fori_loop(1, R - 1, second, 0)

    def third(i, carry):
        au, _ = apply_row(qe, kx, ky, kz, i, shift)
        rm[i] = rm[i] - au
        return carry

    lax.fori_loop(2, R - 2, third, 0)
    cx, cy = nx // 2, ny // 2
    b3 = halve(rm, tmp, MX, MX, cx, cy, 0.5)
    m3 = halve(me, tmp, MX, MX, cx, cy, 0.125)
    both = jnp.concatenate([b3, m3], axis=1)

    def put(k, carry):
        out[k] = both
        return carry

    lax.fori_loop(0, out.shape[0], put, 0)


def finish(pos, got, xm, rm, w2, kx2, ky2, kz2, x1, r1, gxl, gxh, gyl, gyh, w, kx, ky, kz,
           new,
           bc, mc, wc, pc, sc, ec, t1, vm, um, t2, t3, vf, uf):
    X, Y, Z = x1.shape
    nx, ny, nz = X // 2, Y // 2, Z // 2
    cx, cy, cz = nx // 2, ny // 2, nz // 2
    CX, CY = bc.shape[0], bc.shape[1]
    NX, NY = CX // cx, CY // cy
    px, py = pos[0], pos[1]

    def place(k, carry):
        gx = lax.rem(px + k + NX - 1, NX)
        for l in range(NY):
            gy = lax.rem(py + l + NY - 1, NY)
            part = got[gx * NY + gy]
            bc[pl.ds(k * cx, cx), l * cy:(l + 1) * cy, :] = part[:, 0:cy, :]
            mc[pl.ds(k * cx, cx), l * cy:(l + 1) * cy, :] = part[:, cy:2 * cy, :]
        return carry

    lax.fori_loop(0, NX, place, 0)
    shift = 16.0 * SHIFT

    def plane(f):
        zs = nxt(f, 1) + prv(f, 1)
        c1 = zs + (nxt(f, 0) + prv(f, 0))
        c2 = nxt(zs, 0) + prv(zs, 0)
        return 0.5 * c1 + 0.125 * c2, 0.5 * f + 0.125 * c1 + 0.0625 * c2

    def up(i):
        return lax.rem(i + 1, CX)

    def down(i):
        return lax.rem(i + CX - 1, CX)

    def diag_planes(i, carry):
        a, o = plane(mc[i])
        sc[i] = a
        pc[i] = o
        return carry

    lax.fori_loop(0, CX, diag_planes, 0)

    def diag_rows(i, carry):
        ms = sc[i] + (pc[up(i)] + pc[down(i)])
        d = shift + 0.5 * (WEIGHT_TOTAL * mc[i] + ms)
        wi = JACOBI / d
        wc[i] = wi
        ec[i] = wi * bc[i]
        return carry

    lax.fori_loop(0, CX, diag_rows, 0)

    def sweep(_, carry):
        def planes(i, c):
            e = ec[i]
            a, o = plane(e)
            am, om = plane(mc[i] * e)
            sc[i] = a
            pc[i] = o
            t1[i] = am
            t1[CX + i] = om
            return c

        lax.fori_loop(0, CX, planes, 0)

        def rows(i, c):
            se = sc[i] + (pc[up(i)] + pc[down(i)])
            sm = t1[i] + (t1[CX + up(i)] + t1[CX + down(i)])
            e = ec[i]
            ec[i] = e + (wc[i] * (bc[i] + 0.5 * (mc[i] * se + sm)) - JACOBI * e)
            return c

        return lax.fori_loop(0, CX, rows, carry)

    lax.fori_loop(0, SWEEPS - 1, sweep, 0)
    zero = jnp.zeros((CY, cz), F32)

    def total(i, c):
        return c[0] + bc[i], c[1] + ec[i], c[2] + mc[i]

    sb, se, sm = lax.fori_loop(0, CX, total, (zero, zero, zero))
    scale = 1.0 / (CX * CY * cz)
    mean_b = jnp.sum(jnp.sum(sb, axis=0, keepdims=True), axis=1, keepdims=True) * scale
    mean_e = jnp.sum(jnp.sum(se, axis=0, keepdims=True), axis=1, keepdims=True) * scale
    mean_m = jnp.sum(jnp.sum(sm, axis=0, keepdims=True), axis=1, keepdims=True) * scale
    kappa = JACOBI * (mean_b - shift * mean_e) / (shift + WEIGHT_TOTAL * mean_m)

    ex, ey = cx + 4, cy + 4
    e = ec[cx - 2:cx - 2 + ex] + kappa.reshape(1, 1, 1)
    ed = dot(e.reshape(ex * CY, cz), spread_matrix(cz)).reshape(ex, CY, nz)[:, cy - 2:cy - 2 + ey, :]
    for a in range(ex):
        both = repeat_rows(t2, ed[a])
        vm[2 * a] = both
        vm[2 * a + 1] = both
    R = nx + 2 * MX
    shift = 4.0 * SHIFT

    def mid_first(i, carry):
        au, c = apply_row(vm, kx2, ky2, kz2, i, shift)
        res = rm[i] - au
        upd = (w2[i] * res) * INV_C
        rm[i] = res
        um[i] = upd
        xm[i] = xm[i] + c + upd
        return carry

    lax.fori_loop(2, R - 2, mid_first, 0)

    def mid_second(i, carry):
        au, c = apply_row(um, kx2, ky2, kz2, i, shift)
        xm[i] = xm[i] + (ALPHA * c + BETA * (w2[i] * (rm[i] - au)))
        return carry

    lax.fori_loop(3, R - 3, mid_second, 0)

    ye = Y + 2 * FY
    wide = nx + 2
    big = dot(xm[MX - 1:MX - 1 + wide].reshape(wide * (ny + 2 * MX), nz), spread_matrix(nz))
    big = big.reshape(wide, ny + 2 * MX, Z)[:, MX - 2:MX - 2 + ny + 4, :]
    for a in range(wide):
        both = repeat_rows(t3, big[a])
        vf[1 + 2 * a] = both
        vf[2 + 2 * a] = both
    RF = X + 2 * FX
    uf[FX:FX + X, FY:FY + Y, :] = r1[...]
    for row, msg in ((FX - 1, gxl), (FX + X, gxh)):
        for h in range(2):
            for g in range(2):
                uf[row, FY + h * ny:FY + (h + 1) * ny, g * nz:(g + 1) * nz] = msg[8 + 2 * h + g]
    for colj, msg in ((FY - 1, gyl), (FY + Y, gyh)):
        for h in range(2):
            for k in range(ny):
                for g in range(2):
                    uf[FX + h * ny + k, colj:colj + 1, g * nz:(g + 1) * nz] = msg[nx + 2 * h + g, k:k + 1, :]

    def fine_first(i, carry):
        au, _ = apply_row(vf, kx, ky, kz, i, SHIFT)
        uf[i] = uf[i] - au
        return carry

    lax.fori_loop(2, RF - 2, fine_first, 0)

    def scaled(i):
        return (w[i] * uf[i]) * INV_C

    def fine_second(i, carry):
        down_v, c = carry
        up_v = scaled(i + 1)
        acc = SHIFT * c + kx[i] * (c - up_v) + kx[i - 1] * (c - down_v)
        fy = ky[i] * (c - nxt(c, 0))
        fz = kz[i] * (c - nxt(c, 1))
        au = acc + (fy - prv(fy, 0)) + (fz - prv(fz, 1))
        upd = ALPHA * c + BETA * (w[i] * (uf[i] - au))
        vf[i] = vf[i] + c + upd
        return c, up_v

    lax.fori_loop(FX, FX + X, fine_second, (scaled(FX - 1), scaled(FX)))
    new[...] = x1[...] + vf[FX:FX + X, FY:FY + Y, :]


def vmem_call(body, name, out_shape, scratch, inputs, smem=0):
    space = pl.BlockSpec(memory_space=pltpu.VMEM)
    specs = [pl.BlockSpec(memory_space=pltpu.SMEM)] * smem + [space] * (len(inputs) - smem)
    single = not isinstance(out_shape, (list, tuple))
    return pl.pallas_call(
        body,
        name=name,
        out_shape=out_shape,
        in_specs=specs,
        out_specs=space if single else [space] * len(out_shape),
        scratch_shapes=scratch,
        compiler_params=pltpu.CompilerParams(vmem_limit_bytes=VMEM_LIMIT),
    )(*inputs)


DIRS = ((1, 0), (-1, 0), (0, 1), (0, -1), (1, 1), (1, -1), (-1, 1), (-1, -1))


def exchange(messages):
    nx, ny = lax.axis_size("gx"), lax.axis_size("gy")
    got = []
    for msg, (dx, dy) in zip(messages, DIRS):
        pairs = [(i * ny + j, ((i + dx) % nx) * ny + (j + dy) % ny) for i in range(nx) for j in range(ny)]
        got.append(lax.ppermute(msg, ("gx", "gy"), pairs))
    return got


def sd(*shape):
    return jax.ShapeDtypeStruct(shape, F32)


def vm(*shape):
    return pltpu.VMEM(shape, F32)


def local(pressure, divergence, inverse_density):
    X, Y, Z = pressure.shape
    nx, ny, nz = X // 2, Y // 2, Z // 2
    cx, cy, cz = nx // 2, ny // 2, nz // 2
    NX, NY = lax.axis_size("gx"), lax.axis_size("gy")
    xe, ye = X + 2 * FX, Y + 2 * FY
    mxe, mye = nx + 2 * MX, ny + 2 * MX
    fine = (pressure, divergence, inverse_density)
    msgs = vmem_call(pack_fine, "pack_fine",
                     [sd(8, Y, Z)] * 2 + [sd(X, 8, Z)] * 2 + [sd(2, 8, Z)] * 4, [], fine)
    got = exchange(msgs)
    res = vmem_call(
        smooth_fine, "smooth_fine",
        [sd(X, Y, Z)] * 2 + [sd(xe, ye, Z)] * 4 + [sd(nx, ny, nz)] * 2
        + [sd(12, ny, nz)] * 2 + [sd(nx + 4, 8, nz)] * 2 + [sd(4, 8, nz)] * 4,
        [vm(xe, ye, Z)] * 5 + [vm(nx + 2, Z // LANES, ye, LANES)],
        fine + tuple(got))
    x1, r1, w, kx, ky, kz, b2, m2 = res[:8]
    got2 = exchange(res[8:])
    xm, rm, w2, kx2, ky2, kz2, out = vmem_call(
        smooth_mid, "smooth_mid",
        [sd(mxe, mye, nz)] * 6 + [sd(NX * NY, cx, 2 * cy, cz)],
        [vm(mxe, mye, nz)] * 3 + [vm(cx, nz // LANES, mye, LANES)],
        (b2, m2) + tuple(got2))
    gathered = lax.all_to_all(out, ("gx", "gy"), 0, 0)
    pos = jnp.stack([lax.axis_index("gx"), lax.axis_index("gy")]).astype(jnp.int32)
    CX, CY = NX * cx, NY * cy
    return vmem_call(
        finish, "finish", sd(X, Y, Z),
        [vm(CX, CY, cz)] * 6 + [vm(2 * CX, CY, cz)] + [vm(mxe, mye, nz)] * 2 + [vm(nz // LANES, mye, LANES), vm(Z // LANES, ye, LANES)] + [vm(xe, ye, Z)] * 2,
        (pos, gathered, xm, rm, w2, kx2, ky2, kz2, x1, r1) + tuple(got2[:4]) + (w, kx, ky, kz), smem=1)


def solution(mesh):
    return jax.shard_map(
        local,
        mesh=mesh,
        in_specs=(P("gx", "gy", None),) * 3,
        out_specs=P("gx", "gy", None),
        check_vma=False,
    )
```

```python
import jax
import jax.numpy as jnp
from jax import lax
from jax.experimental import pallas as pl
from jax.experimental.pallas import tpu as pltpu
from jax.sharding import PartitionSpec as P

SWEEPS = 4
SHIFT = 0.05
CENTER = (2.0 + 0.3) / 2
HALF = (2.0 - 0.3) / 2
Q0 = CENTER / HALF
P0 = 1.0 / Q0
P1 = 1.0 / (2.0 * Q0 - P0)
ALPHA = P1 * P0
BETA = 2.0 * P1 / HALF
INV_C = 1.0 / CENTER
JACOBI = 0.8
WEIGHT_TOTAL = 5.0

FX = 3
FY = 4
MX = 4

F32 = jnp.float32
UF = 4
UM = 7
UC = 8
VMEM_LIMIT = 20 * 1024 * 1024


def nxt(v, axis):
    return pltpu.roll(v, v.shape[axis] - 1, axis)


def prv(v, axis):
    return pltpu.roll(v, 1, axis)


def loop(low, high, body, init, unroll):
    rest = (high - low) % unroll
    carry = init
    for k in range(rest):
        carry = body(low + k, carry)
    start = low + rest

    def group(g, c):
        for k in range(unroll):
            c = body(start + g * unroll + k, c)
        return c

    return lax.fori_loop(0, (high - start) // unroll, group, carry)


def coefficients(m_ref, k, rows, shift, unroll):
    kx, ky, kyp, kz, kzp, d_ref, w_ref = k
    kx[0] = 0.5 * (m_ref[0] + m_ref[1])

    def body(i, carry):
        m = m_ref[i]
        fx = 0.5 * (m + m_ref[i + 1])
        fxp = 0.5 * (m + m_ref[i - 1])
        fz = 0.5 * (m + nxt(m, 1))
        fzp = 0.5 * (m + prv(m, 1))
        fy = 0.5 * (m + nxt(m, 0))
        fyp = 0.5 * (m + prv(m, 0))
        kx[i] = fx
        ky[i] = fy
        kyp[i] = fyp
        kz[i] = fz
        kzp[i] = fzp
        d = shift + ((fx + fxp) + (fy + fyp) + (fz + fzp))
        d_ref[i] = d
        w_ref[i] = 1.0 / d
        return carry

    loop(1, rows - 1, body, 0, unroll)


def apply_row(v_ref, k, i):
    kx, ky, kyp, kz, kzp, d_ref, w_ref = k
    c = v_ref[i]
    z = kz[i] * nxt(c, 1) + kzp[i] * prv(c, 1)
    y = ky[i] * nxt(c, 0) + kyp[i] * prv(c, 0)
    x = kx[i] * v_ref[i + 1] + kx[i - 1] * v_ref[i - 1]
    return d_ref[i] * c - ((x + y) + z), c


def dot(a, b):
    return jnp.dot(a, b, precision=lax.Precision.HIGHEST, preferred_element_type=F32)


def pair_matrix(z, value):
    row = lax.broadcasted_iota(jnp.int32, (z, z // 2), 0)
    col = lax.broadcasted_iota(jnp.int32, (z, z // 2), 1)
    return jnp.where(row // 2 == col, value, 0.0).astype(F32)


def spread_matrix(z):
    row = lax.broadcasted_iota(jnp.int32, (z, 2 * z), 0)
    col = lax.broadcasted_iota(jnp.int32, (z, 2 * z), 1)
    return jnp.where(col // 2 == row, 1.0, 0.0).astype(F32)


LANES = 128


def put_lanes(tmp, a, val):
    for g in range(val.shape[1] // LANES):
        tmp[a, g] = val[:, g * LANES:(g + 1) * LANES]


def take_pairs(tmp, a, y0, ny, chunks):
    parts = [tmp[a, g, pl.ds(y0, ny, stride=2), :] + tmp[a, g, pl.ds(y0 + 1, ny, stride=2), :] for g in range(chunks)]
    return jnp.concatenate(parts, axis=1)


def repeat_rows(tmp, val):
    n, chunks = val.shape[0], val.shape[1] // LANES
    for g in range(chunks):
        part = val[:, g * LANES:(g + 1) * LANES]
        tmp[g, pl.ds(0, n, stride=2), :] = part
        tmp[g, pl.ds(1, n, stride=2), :] = part
    return jnp.concatenate([tmp[g] for g in range(chunks)], axis=1)


def halve(ref, tmp, x0, y0, nx, ny, value):
    z = ref.shape[2]
    for a in range(nx):
        put_lanes(tmp, a, ref[x0 + 2 * a] + ref[x0 + 2 * a + 1])
    s = jnp.concatenate([take_pairs(tmp, a, y0, ny, z // LANES) for a in range(nx)], axis=0)
    return dot(s, pair_matrix(z, value)).reshape(nx, ny, z // 2)


def pack_fine(x, b, m, *outs):
    X, Y = x.shape[0], x.shape[1]
    gxp, gxm, gyp, gym, cpp, cpm, cmp_, cmm = outs
    for out, sl in ((gxp, lambda k: slice(X - k, X)), (gxm, lambda k: slice(0, k))):
        out[0:3] = x[sl(3)]
        out[3:5] = b[sl(2)]
        out[5:8] = m[sl(3)]
    for out, sl in ((gyp, lambda k: slice(Y - k, Y)), (gym, lambda k: slice(0, k))):
        out[:, 0:3, :] = x[:, sl(3), :]
        out[:, 3:5, :] = b[:, sl(2), :]
        out[:, 5:8, :] = m[:, sl(3), :]
    for out, sx, sy in ((cpp, 1, 1), (cpm, 1, -1), (cmp_, -1, 1), (cmm, -1, -1)):
        rows = slice(X - 2, X) if sx > 0 else slice(0, 2)
        cols = slice(Y - 2, Y) if sy > 0 else slice(0, 2)
        out[:, 0:2, :] = x[rows, cols, :]
        out[:, 2:4, :] = b[rows, cols, :]
        out[:, 4:6, :] = m[rows, cols, :]
        out[:, 6:8, :] = m[rows, cols, :]


def smooth_fine(x, b, m, gxl, gxh, gyl, gyh, cll, clh, chl, chh,
                x1, r1, kx, ky, kyp, kz, kzp, dg, w, b2, m2, sxp, sxm, syp, sym, spp, spm, smp, smm,
                xe, be, me, u, r, tmp):
    X, Y, Z = x.shape
    R = X + 2 * FX
    x_end, y_end = FX + X, FY + Y
    for ext, own, lo, n in ((xe, x, 0, 3), (be, b, 3, 2), (me, m, 5, 3)):
        ext[FX:x_end, FY:y_end, :] = own[...]
        ext[FX - n:FX, FY:y_end, :] = gxl[lo:lo + n]
        ext[x_end:x_end + n, FY:y_end, :] = gxh[lo:lo + n]
        ext[FX:x_end, FY - n:FY, :] = gyl[:, lo:lo + n, :]
        ext[FX:x_end, y_end:y_end + n, :] = gyh[:, lo:lo + n, :]
    for msg, rows, cols in ((cll, slice(FX - 2, FX), slice(FY - 2, FY)),
                            (clh, slice(FX - 2, FX), slice(y_end, y_end + 2)),
                            (chl, slice(x_end, x_end + 2), slice(FY - 2, FY)),
                            (chh, slice(x_end, x_end + 2), slice(y_end, y_end + 2))):
        xe[rows, cols, :] = msg[:, 0:2, :]
        be[rows, cols, :] = msg[:, 2:4, :]
        me[rows, cols, :] = msg[:, 4:6, :]
    co = (kx, ky, kyp, kz, kzp, dg, w)
    coefficients(me, co, R, SHIFT, UF)

    def first(i, carry):
        ax, _ = apply_row(xe, co, i)
        res = be[i] - ax
        r[i] = res
        u[i] = (w[i] * res) * INV_C
        return carry

    loop(1, R - 1, first, 0, UF)

    def second(i, carry):
        au, c = apply_row(u, co, i)
        res = r[i] - au
        r[i] = res
        up = ALPHA * c + BETA * (w[i] * res)
        xe[i] = xe[i] + c + up
        be[i] = up
        return carry

    loop(2, R - 2, second, 0, UF)

    def third(i, carry):
        au, _ = apply_row(be, co, i)
        r[i] = r[i] - au
        return carry

    loop(3, R - 3, third, 0, UF)
    x1[...] = xe[FX:x_end, FY:y_end, :]
    r1[...] = r[FX:x_end, FY:y_end, :]
    nx, ny, nz = X // 2, Y // 2, Z // 2
    b2[...] = halve(r, tmp, FX, FY, nx, ny, 0.5)
    mm = halve(me, tmp, FX - 2, 0, nx + 2, ny + 4, 0.125)
    cells = mm[1:nx + 1, 2:2 + ny, :]
    m2[...] = cells
    fz = 0.5 * (cells + nxt(cells, 2))
    fzp = prv(fz, 2)
    diag = (4.0 * SHIFT + 0.5 * (4.0 * cells + mm[0:nx, 2:2 + ny, :] + mm[2:nx + 2, 2:2 + ny, :]
                                 + mm[1:nx + 1, 1:1 + ny, :] + mm[1:nx + 1, 3:3 + ny, :]) + (fz + fzp))
    u2 = (b2[...] * (1.0 / diag)) * INV_C
    bb = b2[...]
    sxp[0:1] = u2[nx - 4:nx - 3]
    sxp[1:4] = bb[nx - 3:nx]
    sxp[4:8] = cells[nx - 4:nx]
    sxm[0:3] = bb[0:3]
    sxm[3:4] = u2[3:4]
    sxm[4:8] = cells[0:4]
    syp[0:nx, 0:1, :] = u2[:, ny - 4:ny - 3, :]
    syp[0:nx, 1:4, :] = bb[:, ny - 3:ny, :]
    syp[0:nx, 4:8, :] = cells[:, ny - 4:ny, :]
    sym[0:nx, 0:3, :] = bb[:, 0:3, :]
    sym[0:nx, 3:4, :] = u2[:, 3:4, :]
    sym[0:nx, 4:8, :] = cells[:, 0:4, :]
    for dst, src in ((sxp, r1[X - 1]), (sxm, r1[0])):
        for h in range(2):
            for g in range(2):
                dst[8 + 2 * h + g] = src[h * ny:(h + 1) * ny, g * nz:(g + 1) * nz]
    for dst, j in ((syp, Y - 1), (sym, 0)):
        for h in range(2):
            for k in range(ny):
                row = r1[h * ny + k, j:j + 1, :]
                for g in range(2):
                    dst[nx + 2 * h + g, k:k + 1, :] = row[:, g * nz:(g + 1) * nz]
    for out, sx, sy in ((spp, 1, 1), (spm, 1, -1), (smp, -1, 1), (smm, -1, -1)):
        for k in range(4):
            i = nx - 4 + k if sx > 0 else k
            di = 4 - k if sx > 0 else k + 1
            for l in range(4):
                j = ny - 4 + l if sy > 0 else l
                dj = 4 - l if sy > 0 else l + 1
                val = u2 if di + dj == 5 else bb
                out[k, l:l + 1, :] = val[i, j:j + 1, :]
                out[k, 4 + l:5 + l, :] = cells[i, j:j + 1, :]


def smooth_mid(b2, m2, gxl, gxh, gyl, gyh, cll, clh, chl, chh,
               xm, rm, kx, ky, kyp, kz, kzp, dg, w, out,
               qe, me, u, tmp):
    nx, ny, nz = b2.shape
    R = nx + 2 * MX
    shift = 4.0 * SHIFT
    xend, yend = MX + nx, MX + ny
    for ext, own, lo in ((qe, b2, 0), (me, m2, 4)):
        ext[MX:xend, MX:yend, :] = own[...]
        ext[0:MX, MX:yend, :] = gxl[lo:lo + 4]
        ext[xend:xend + MX, MX:yend, :] = gxh[lo:lo + 4]
        ext[MX:xend, 0:MX, :] = gyl[0:nx, lo:lo + 4, :]
        ext[MX:xend, yend:yend + MX, :] = gyh[0:nx, lo:lo + 4, :]
        for msg, rows, cols in ((cll, slice(0, MX), slice(0, MX)),
                                (clh, slice(0, MX), slice(yend, yend + MX)),
                                (chl, slice(xend, xend + MX), slice(0, MX)),
                                (chh, slice(xend, xend + MX), slice(yend, yend + MX))):
            ext[rows, cols, :] = msg[:, lo:lo + 4, :]
    co = (kx, ky, kyp, kz, kzp, dg, w)
    coefficients(me, co, R, shift, UM)
    col = lax.broadcasted_iota(jnp.int32, (ny + 2 * MX, nz), 0)
    dcol = jnp.maximum(jnp.maximum(MX - col, col - (yend - 1)), 0)

    def first(i, carry):
        di = jnp.maximum(jnp.maximum(MX - i, i - (xend - 1)), 0)
        q = qe[i]
        sent = (dcol + di == 5) | (dcol == 4) | (di == 4)
        u[i] = jnp.where(sent, q, (w[i] * q) * INV_C)
        return carry

    u[0] = qe[0]
    u[R - 1] = qe[R - 1]
    loop(1, R - 1, first, 0, UM)

    def second(i, carry):
        au, c = apply_row(u, co, i)
        res = qe[i] - au
        rm[i] = res
        up = ALPHA * c + BETA * (w[i] * res)
        xm[i] = c + up
        qe[i] = up
        return carry

    loop(1, R - 1, second, 0, UM)

    def third(i, carry):
        au, _ = apply_row(qe, co, i)
        rm[i] = rm[i] - au
        return carry

    loop(2, R - 2, third, 0, UM)
    cx, cy = nx // 2, ny // 2
    b3 = halve(rm, tmp, MX, MX, cx, cy, 0.5)
    m3 = halve(me, tmp, MX, MX, cx, cy, 0.125)
    both = jnp.concatenate([b3, m3], axis=1)

    def put(k, carry):
        out[k] = both
        return carry

    lax.fori_loop(0, out.shape[0], put, 0)


def finish(got, xm, rm, kx2, ky2, kyp2, kz2, kzp2, dg2, w2, x1, r1, gxl, gxh, gyl, gyh,
           kx, ky, kyp, kz, kzp, dg, w, new,
           bc, mc, wc, pc, sc, ec, t1, vm, um, t2, t3, vf, uf, qf):
    X, Y, Z = x1.shape
    nx, ny, nz = X // 2, Y // 2, Z // 2
    cx, cy, cz = nx // 2, ny // 2, nz // 2
    CX, CY = bc.shape[0], bc.shape[1]
    NX, NY = CX // cx, CY // cy
    px, py = lax.axis_index("gx"), lax.axis_index("gy")

    def place(k, carry):
        gx = lax.rem(px + k + NX - 1, NX)
        for l in range(NY):
            gy = lax.rem(py + l + NY - 1, NY)
            part = got[gx * NY + gy]
            bc[pl.ds(k * cx, cx), l * cy:(l + 1) * cy, :] = part[:, 0:cy, :]
            mc[pl.ds(k * cx, cx), l * cy:(l + 1) * cy, :] = part[:, cy:2 * cy, :]
        return carry

    lax.fori_loop(0, NX, place, 0)
    shift = 16.0 * SHIFT

    def plane(f):
        zs = nxt(f, 1) + prv(f, 1)
        c1 = zs + (nxt(f, 0) + prv(f, 0))
        c2 = nxt(zs, 0) + prv(zs, 0)
        return 0.5 * c1 + 0.125 * c2, 0.5 * f + 0.125 * c1 + 0.0625 * c2

    def up(i):
        return lax.rem(i + 1, CX)

    def down(i):
        return lax.rem(i + CX - 1, CX)

    def diag_planes(i, carry):
        a, o = plane(mc[i])
        sc[i] = a
        pc[i] = o
        return carry

    loop(0, CX, diag_planes, 0, UC)

    def diag_rows(i, carry):
        ms = sc[i] + (pc[up(i)] + pc[down(i)])
        d = shift + 0.5 * (WEIGHT_TOTAL * mc[i] + ms)
        wi = JACOBI / d
        wc[i] = wi
        ec[i] = wi * bc[i]
        return carry

    loop(0, CX, diag_rows, 0, UC)

    def sweep(_, carry):
        def planes(i, c):
            e = ec[i]
            a, o = plane(e)
            am, om = plane(mc[i] * e)
            sc[i] = a
            pc[i] = o
            t1[i] = am
            t1[CX + i] = om
            return c

        loop(0, CX, planes, 0, UC)

        def rows(i, c):
            se = sc[i] + (pc[up(i)] + pc[down(i)])
            sm = t1[i] + (t1[CX + up(i)] + t1[CX + down(i)])
            e = ec[i]
            ec[i] = e + (wc[i] * (bc[i] + 0.5 * (mc[i] * se + sm)) - JACOBI * e)
            return c

        return loop(0, CX, rows, carry, UC)

    lax.fori_loop(0, SWEEPS - 1, sweep, 0)
    zero = jnp.zeros((CY, cz), F32)

    def total(i, c):
        return c[0] + bc[i], c[1] + ec[i], c[2] + mc[i]

    sb, se, sm = loop(0, CX, total, (zero, zero, zero), UC)
    scale = 1.0 / (CX * CY * cz)
    mean_b = jnp.sum(jnp.sum(sb, axis=0, keepdims=True), axis=1, keepdims=True) * scale
    mean_e = jnp.sum(jnp.sum(se, axis=0, keepdims=True), axis=1, keepdims=True) * scale
    mean_m = jnp.sum(jnp.sum(sm, axis=0, keepdims=True), axis=1, keepdims=True) * scale
    kappa = JACOBI * (mean_b - shift * mean_e) / (shift + WEIGHT_TOTAL * mean_m)

    ex, ey = cx + 4, cy + 4
    e = ec[cx - 2:cx - 2 + ex] + kappa.reshape(1, 1, 1)
    ed = dot(e.reshape(ex * CY, cz), spread_matrix(cz)).reshape(ex, CY, nz)[:, cy - 2:cy - 2 + ey, :]
    for a in range(ex):
        both = repeat_rows(t2, ed[a])
        vm[2 * a] = both
        vm[2 * a + 1] = both
    R = nx + 2 * MX
    co2 = (kx2, ky2, kyp2, kz2, kzp2, dg2, w2)
    co = (kx, ky, kyp, kz, kzp, dg, w)

    def mid_first(i, carry):
        au, c = apply_row(vm, co2, i)
        res = rm[i] - au
        upd = (w2[i] * res) * INV_C
        rm[i] = res
        um[i] = upd
        xm[i] = xm[i] + c + upd
        return carry

    loop(2, R - 2, mid_first, 0, UM)

    def mid_second(i, carry):
        au, c = apply_row(um, co2, i)
        xm[i] = xm[i] + (ALPHA * c + BETA * (w2[i] * (rm[i] - au)))
        return carry

    loop(3, R - 3, mid_second, 0, UM)

    ye = Y + 2 * FY
    wide = nx + 2
    big = dot(xm[MX - 1:MX - 1 + wide].reshape(wide * (ny + 2 * MX), nz), spread_matrix(nz))
    big = big.reshape(wide, ny + 2 * MX, Z)[:, MX - 2:MX - 2 + ny + 4, :]
    for a in range(wide):
        both = repeat_rows(t3, big[a])
        vf[1 + 2 * a] = both
        vf[2 + 2 * a] = both
    RF = X + 2 * FX
    uf[FX:FX + X, FY:FY + Y, :] = r1[...]
    for row, msg in ((FX - 1, gxl), (FX + X, gxh)):
        for h in range(2):
            for g in range(2):
                uf[row, FY + h * ny:FY + (h + 1) * ny, g * nz:(g + 1) * nz] = msg[8 + 2 * h + g]
    for colj, msg in ((FY - 1, gyl), (FY + Y, gyh)):
        for h in range(2):
            for k in range(ny):
                for g in range(2):
                    uf[FX + h * ny + k, colj:colj + 1, g * nz:(g + 1) * nz] = msg[nx + 2 * h + g, k:k + 1, :]

    def fine_first(i, carry):
        au, _ = apply_row(vf, co, i)
        res = uf[i] - au
        uf[i] = res
        qf[i] = (w[i] * res) * INV_C
        return carry

    loop(2, RF - 2, fine_first, 0, UF)

    def fine_second(i, carry):
        au, c = apply_row(qf, co, i)
        uf[i] = vf[i] + ((1.0 + ALPHA) * c + BETA * (w[i] * (uf[i] - au)))
        return carry

    loop(FX, FX + X, fine_second, 0, UF)
    new[...] = x1[...] + uf[FX:FX + X, FY:FY + Y, :]


def vmem_call(body, name, out_shape, scratch, inputs):
    space = pl.BlockSpec(memory_space=pltpu.VMEM)
    single = not isinstance(out_shape, (list, tuple))
    return pl.pallas_call(
        body,
        name=name,
        out_shape=out_shape,
        in_specs=[space] * len(inputs),
        out_specs=space if single else [space] * len(out_shape),
        scratch_shapes=scratch,
        compiler_params=pltpu.CompilerParams(vmem_limit_bytes=VMEM_LIMIT),
    )(*inputs)


DIRS = ((1, 0), (-1, 0), (0, 1), (0, -1), (1, 1), (1, -1), (-1, 1), (-1, -1))


def exchange(messages):
    nx, ny = lax.axis_size("gx"), lax.axis_size("gy")
    got = []
    for msg, (dx, dy) in zip(messages, DIRS):
        pairs = [(i * ny + j, ((i + dx) % nx) * ny + (j + dy) % ny) for i in range(nx) for j in range(ny)]
        got.append(lax.ppermute(msg, ("gx", "gy"), pairs))
    return got


def sd(*shape):
    return jax.ShapeDtypeStruct(shape, F32)


def vm(*shape):
    return pltpu.VMEM(shape, F32)


def local(pressure, divergence, inverse_density):
    X, Y, Z = pressure.shape
    nx, ny, nz = X // 2, Y // 2, Z // 2
    cx, cy, cz = nx // 2, ny // 2, nz // 2
    NX, NY = lax.axis_size("gx"), lax.axis_size("gy")
    xe, ye = X + 2 * FX, Y + 2 * FY
    mxe, mye = nx + 2 * MX, ny + 2 * MX
    fine = (pressure, divergence, inverse_density)
    msgs = vmem_call(pack_fine, "pack_fine",
                     [sd(8, Y, Z)] * 2 + [sd(X, 8, Z)] * 2 + [sd(2, 8, Z)] * 4, [], fine)
    got = exchange(msgs)
    res = vmem_call(
        smooth_fine, "smooth_fine",
        [sd(X, Y, Z)] * 2 + [sd(xe, ye, Z)] * 7 + [sd(nx, ny, nz)] * 2
        + [sd(12, ny, nz)] * 2 + [sd(nx + 4, 8, nz)] * 2 + [sd(4, 8, nz)] * 4,
        [vm(xe, ye, Z)] * 5 + [vm(nx + 2, Z // LANES, ye, LANES)],
        fine + tuple(got))
    x1, r1 = res[:2]
    fine_co = tuple(res[2:9])
    b2, m2 = res[9:11]
    got2 = exchange(res[11:])
    *mid, out = vmem_call(
        smooth_mid, "smooth_mid",
        [sd(mxe, mye, nz)] * 9 + [sd(NX * NY, cx, 2 * cy, cz)],
        [vm(mxe, mye, nz)] * 3 + [vm(cx, nz // LANES, mye, LANES)],
        (b2, m2) + tuple(got2))
    gathered = lax.all_to_all(out, ("gx", "gy"), 0, 0)
    CX, CY = NX * cx, NY * cy
    return vmem_call(
        finish, "finish", sd(X, Y, Z),
        [vm(CX, CY, cz)] * 6 + [vm(2 * CX, CY, cz)] + [vm(mxe, mye, nz)] * 2 + [vm(nz // LANES, mye, LANES), vm(Z // LANES, ye, LANES)] + [vm(xe, ye, Z)] * 3,
        (gathered, *mid, x1, r1) + tuple(got2[:4]) + fine_co)


def solution(mesh):
    return jax.shard_map(
        local,
        mesh=mesh,
        in_specs=(P("gx", "gy", None),) * 3,
        out_specs=P("gx", "gy", None),
        check_vma=False,
    )
```

```python
import jax
import jax.numpy as jnp
from jax import lax
from jax.experimental import pallas as pl
from jax.experimental.pallas import tpu as pltpu
from jax.sharding import PartitionSpec as P

SWEEPS = 4
SHIFT = 0.05
CENTER = (2.0 + 0.3) / 2
HALF = (2.0 - 0.3) / 2
Q0 = CENTER / HALF
P0 = 1.0 / Q0
P1 = 1.0 / (2.0 * Q0 - P0)
ALPHA = P1 * P0
BETA = 2.0 * P1 / HALF
INV_C = 1.0 / CENTER
JACOBI = 0.8
WEIGHT_TOTAL = 5.0

FX = 3
FY = 4
MX = 4

F32 = jnp.float32
UF = 4
UM = 7
UC = 8
PIECES = 4
VMEM_LIMIT = 20 * 1024 * 1024


def nxt(v, axis):
    return pltpu.roll(v, v.shape[axis] - 1, axis)


def prv(v, axis):
    return pltpu.roll(v, 1, axis)


def loop(low, high, body, init, unroll):
    rest = (high - low) % unroll
    carry = init
    for k in range(rest):
        carry = body(low + k, carry)
    start = low + rest

    def group(g, c):
        for k in range(unroll):
            c = body(start + g * unroll + k, c)
        return c

    return lax.fori_loop(0, (high - start) // unroll, group, carry)


def coefficients(m_ref, k, rows, shift, unroll):
    kx, ky, kyp, kz, kzp, d_ref, w_ref = k
    kx[0] = 0.5 * (m_ref[0] + m_ref[1])

    def body(i, carry):
        m = m_ref[i]
        fx = 0.5 * (m + m_ref[i + 1])
        fxp = 0.5 * (m + m_ref[i - 1])
        fz = 0.5 * (m + nxt(m, 1))
        fzp = 0.5 * (m + prv(m, 1))
        fy = 0.5 * (m + nxt(m, 0))
        fyp = 0.5 * (m + prv(m, 0))
        kx[i] = fx
        ky[i] = fy
        kyp[i] = fyp
        kz[i] = fz
        kzp[i] = fzp
        d = shift + ((fx + fxp) + (fy + fyp) + (fz + fzp))
        d_ref[i] = d
        w_ref[i] = 1.0 / d
        return carry

    loop(1, rows - 1, body, 0, unroll)


def apply_row(v_ref, k, i):
    kx, ky, kyp, kz, kzp, d_ref, w_ref = k
    c = v_ref[i]
    z = kz[i] * nxt(c, 1) + kzp[i] * prv(c, 1)
    y = ky[i] * nxt(c, 0) + kyp[i] * prv(c, 0)
    x = kx[i] * v_ref[i + 1] + kx[i - 1] * v_ref[i - 1]
    return d_ref[i] * c - ((x + y) + z), c


BF16 = jnp.bfloat16


def select(a, table):
    hi = a.astype(BF16)
    rest = a - hi.astype(F32)
    mid = rest.astype(BF16)
    low = (rest - mid.astype(F32)).astype(BF16)
    n = a.shape[0]
    out = jnp.dot(jnp.concatenate([hi, mid, low], axis=0), table, preferred_element_type=F32)
    return (out[0:n] + out[n:2 * n]) + out[2 * n:3 * n]


def chunks_as_rows(a, width):
    return jnp.concatenate([a[:, g * width:(g + 1) * width] for g in range(a.shape[1] // width)], axis=0)


def rows_as_chunks(a, count):
    n = a.shape[0] // count
    return jnp.concatenate([a[g * n:(g + 1) * n] for g in range(count)], axis=1)


def add_pairs(a):
    row = lax.broadcasted_iota(jnp.int32, (2 * LANES, LANES), 0)
    col = lax.broadcasted_iota(jnp.int32, (2 * LANES, LANES), 1)
    table = jnp.where(row // 2 == col, 1.0, 0.0).astype(BF16)
    return rows_as_chunks(select(chunks_as_rows(a, 2 * LANES), table), a.shape[1] // (2 * LANES))


def double(a):
    row = lax.broadcasted_iota(jnp.int32, (LANES, 2 * LANES), 0)
    col = lax.broadcasted_iota(jnp.int32, (LANES, 2 * LANES), 1)
    table = jnp.where(col // 2 == row, 1.0, 0.0).astype(BF16)
    return rows_as_chunks(select(chunks_as_rows(a, LANES), table), a.shape[1] // LANES)


LANES = 128


def put_lanes(tmp, a, val):
    for g in range(val.shape[1] // LANES):
        tmp[a, g] = val[:, g * LANES:(g + 1) * LANES]


def take_pairs(tmp, a, y0, ny, chunks):
    parts = [tmp[a, g, pl.ds(y0, ny, stride=2), :] + tmp[a, g, pl.ds(y0 + 1, ny, stride=2), :] for g in range(chunks)]
    return jnp.concatenate(parts, axis=1)


def repeat_rows(tmp, val):
    n, chunks = val.shape[0], val.shape[1] // LANES
    for g in range(chunks):
        part = val[:, g * LANES:(g + 1) * LANES]
        tmp[g, pl.ds(0, n, stride=2), :] = part
        tmp[g, pl.ds(1, n, stride=2), :] = part
    return jnp.concatenate([tmp[g] for g in range(chunks)], axis=1)


def pair_rows(ref, tmp, x0, y0, nx, ny):
    z = ref.shape[2]
    for a in range(nx):
        put_lanes(tmp, a, ref[x0 + 2 * a] + ref[x0 + 2 * a + 1])
    return jnp.concatenate([take_pairs(tmp, a, y0, ny, z // LANES) for a in range(nx)], axis=0)


def pack_fine(x_in, b_in, m_in, x, b, m, *outs):
    X, Y = x.shape[0], x.shape[1]
    *outs, sems = outs
    copies = []
    for src, dst in ((x_in, x), (b_in, b), (m_in, m)):
        for k in range(PIECES):
            part = pl.ds(k * (X // PIECES), X // PIECES)
            copies.append(pltpu.make_async_copy(src.at[part], dst.at[part], sems.at[len(copies)]))
    for copy in copies:
        copy.start()
    for copy in copies:
        copy.wait()
    gyp, gym, gxp, gxm, cpp, cpm, cmp_, cmm = outs
    for out, sl in ((gxp, lambda k: slice(X - k, X)), (gxm, lambda k: slice(0, k))):
        out[0:3] = x[sl(3)]
        out[3:5] = b[sl(2)]
        out[5:8] = m[sl(3)]
    for out, sl in ((gyp, lambda k: slice(Y - k, Y)), (gym, lambda k: slice(0, k))):
        out[:, 0:3, :] = x[:, sl(3), :]
        out[:, 3:5, :] = b[:, sl(2), :]
        out[:, 5:8, :] = m[:, sl(3), :]
    for out, sx, sy in ((cpp, 1, 1), (cpm, 1, -1), (cmp_, -1, 1), (cmm, -1, -1)):
        rows = slice(X - 2, X) if sx > 0 else slice(0, 2)
        cols = slice(Y - 2, Y) if sy > 0 else slice(0, 2)
        out[:, 0:2, :] = x[rows, cols, :]
        out[:, 2:4, :] = b[rows, cols, :]
        out[:, 4:6, :] = m[rows, cols, :]
        out[:, 6:8, :] = m[rows, cols, :]


def smooth_fine(x, b, m, gyl, gyh, gxl, gxh, cll, clh, chl, chh,
                xe, r, kx, ky, kyp, kz, kzp, dg, w, b2, m2, sxp, sxm, syp, sym,
                be, me, u, tmp, tmp2):
    X, Y, Z = x.shape
    R = X + 2 * FX
    x_end, y_end = FX + X, FY + Y
    for ext, own, lo, n in ((xe, x, 0, 3), (be, b, 3, 2), (me, m, 5, 3)):
        ext[FX:x_end, FY:y_end, :] = own[...]
        ext[FX - n:FX, FY:y_end, :] = gxl[lo:lo + n]
        ext[x_end:x_end + n, FY:y_end, :] = gxh[lo:lo + n]
        ext[FX:x_end, FY - n:FY, :] = gyl[:, lo:lo + n, :]
        ext[FX:x_end, y_end:y_end + n, :] = gyh[:, lo:lo + n, :]
    for msg, rows, cols in ((cll, slice(FX - 2, FX), slice(FY - 2, FY)),
                            (clh, slice(FX - 2, FX), slice(y_end, y_end + 2)),
                            (chl, slice(x_end, x_end + 2), slice(FY - 2, FY)),
                            (chh, slice(x_end, x_end + 2), slice(y_end, y_end + 2))):
        xe[rows, cols, :] = msg[:, 0:2, :]
        be[rows, cols, :] = msg[:, 2:4, :]
        me[rows, cols, :] = msg[:, 4:6, :]
    co = (kx, ky, kyp, kz, kzp, dg, w)
    coefficients(me, co, R, SHIFT, UF)

    def first(i, carry):
        ax, _ = apply_row(xe, co, i)
        res = be[i] - ax
        r[i] = res
        u[i] = (w[i] * res) * INV_C
        return carry

    loop(1, R - 1, first, 0, UF)

    def second(i, carry):
        au, c = apply_row(u, co, i)
        res = r[i] - au
        r[i] = res
        up = ALPHA * c + BETA * (w[i] * res)
        xe[i] = xe[i] + c + up
        be[i] = up
        return carry

    loop(2, R - 2, second, 0, UF)

    def third(i, carry):
        au, _ = apply_row(be, co, i)
        r[i] = r[i] - au
        return carry

    loop(3, R - 3, third, 0, UF)
    nx, ny, nz = X // 2, Y // 2, Z // 2
    sums = jnp.concatenate([pair_rows(r, tmp, FX, FY, nx, ny), pair_rows(me, tmp2, FX - 2, 0, nx + 2, ny + 4)], axis=0)
    sums = add_pairs(sums)
    b2[...] = 0.5 * sums[0:nx * ny].reshape(nx, ny, nz)
    mm = 0.125 * sums[nx * ny:].reshape(nx + 2, ny + 4, nz)
    cells = mm[1:nx + 1, 2:2 + ny, :]
    m2[...] = cells
    fz = 0.5 * (cells + nxt(cells, 2))
    fzp = prv(fz, 2)
    diag = (4.0 * SHIFT + 0.5 * (4.0 * cells + mm[0:nx, 2:2 + ny, :] + mm[2:nx + 2, 2:2 + ny, :]
                                 + mm[1:nx + 1, 1:1 + ny, :] + mm[1:nx + 1, 3:3 + ny, :]) + (fz + fzp))
    u2 = (b2[...] * (1.0 / diag)) * INV_C
    bb = b2[...]
    sxp[0:1] = u2[nx - 4:nx - 3]
    sxp[1:4] = bb[nx - 3:nx]
    sxp[4:8] = cells[nx - 4:nx]
    sxm[0:3] = bb[0:3]
    sxm[3:4] = u2[3:4]
    sxm[4:8] = cells[0:4]
    syp[0:nx, 0:1, :] = u2[:, ny - 4:ny - 3, :]
    syp[0:nx, 1:4, :] = bb[:, ny - 3:ny, :]
    syp[0:nx, 4:8, :] = cells[:, ny - 4:ny, :]
    sym[0:nx, 0:3, :] = bb[:, 0:3, :]
    sym[0:nx, 3:4, :] = u2[:, 3:4, :]
    sym[0:nx, 4:8, :] = cells[:, 0:4, :]
    for dst, src in ((sxp, r[FX + X - 1, FY:y_end]), (sxm, r[FX, FY:y_end])):
        for h in range(2):
            for g in range(2):
                dst[8 + 2 * h + g] = src[h * ny:(h + 1) * ny, g * nz:(g + 1) * nz]
    for dst, j in ((syp, Y - 1), (sym, 0)):
        for h in range(2):
            for k in range(ny):
                row = r[FX + h * ny + k, FY + j:FY + j + 1, :]
                for g in range(2):
                    dst[nx + 2 * h + g, k:k + 1, :] = row[:, g * nz:(g + 1) * nz]
    for out, j0, step in ((syp, ny - 1, -1), (sym, 0, 1)):
        for t in range(3):
            j = j0 + step * t
            out[nx + 4, t:t + 1, :] = u2[nx - 4 + t, j:j + 1, :]
            out[nx + 4, 3 + t:4 + t, :] = u2[3 - t, j:j + 1, :]


def spread_rows(gyl, gyh, sxp, sxm, axp, axm):
    ny, nx = sxp.shape[1], gyl.shape[0] - 5
    yend = MX + ny
    for own, out, r0, line in ((sxp, axp, nx - 4, 0), (sxm, axm, 0, 3)):
        for lo in (0, 4):
            out[lo:lo + 4, MX:yend, :] = own[lo:lo + 4]
            out[lo:lo + 4, 0:MX, :] = gyl[r0:r0 + 4, lo:lo + 4, :]
            out[lo:lo + 4, yend:yend + MX, :] = gyh[r0:r0 + 4, lo:lo + 4, :]
        for t in range(3):
            row = t if line == 0 else 3 - t
            out[row, 3 - t:4 - t, :] = gyl[nx + 4, line + t:line + t + 1, :]
            out[row, yend + t:yend + t + 1, :] = gyh[nx + 4, line + t:line + t + 1, :]
        for h in range(2):
            for g in range(2):
                out[8 + g, h * ny:(h + 1) * ny, :] = own[8 + 2 * h + g]


def smooth_mid(b2, m2, gxl, gxh, gyl, gyh,
               xm, rm, kx, ky, kyp, kz, kzp, dg, w, out,
               qe, me, u, tmp, tmp2):
    nx, ny, nz = b2.shape
    R = nx + 2 * MX
    shift = 4.0 * SHIFT
    xend, yend = MX + nx, MX + ny
    for ext, own, lo in ((qe, b2, 0), (me, m2, 4)):
        ext[MX:xend, MX:yend, :] = own[...]
        ext[MX:xend, 0:MX, :] = gyl[0:nx, lo:lo + 4, :]
        ext[MX:xend, yend:yend + MX, :] = gyh[0:nx, lo:lo + 4, :]
        ext[0:MX] = gxl[lo:lo + 4]
        ext[xend:xend + MX] = gxh[lo:lo + 4]
    co = (kx, ky, kyp, kz, kzp, dg, w)
    coefficients(me, co, R, shift, UM)
    col = lax.broadcasted_iota(jnp.int32, (ny + 2 * MX, nz), 0)
    dcol = jnp.maximum(jnp.maximum(MX - col, col - (yend - 1)), 0)

    def first(i, carry):
        di = jnp.maximum(jnp.maximum(MX - i, i - (xend - 1)), 0)
        q = qe[i]
        sent = (dcol + di == 5) | (dcol == 4) | (di == 4)
        u[i] = jnp.where(sent, q, (w[i] * q) * INV_C)
        return carry

    u[0] = qe[0]
    u[R - 1] = qe[R - 1]
    loop(1, R - 1, first, 0, UM)

    def second(i, carry):
        au, c = apply_row(u, co, i)
        res = qe[i] - au
        rm[i] = res
        up = ALPHA * c + BETA * (w[i] * res)
        xm[i] = c + up
        qe[i] = up
        return carry

    loop(1, R - 1, second, 0, UM)

    def third(i, carry):
        au, _ = apply_row(qe, co, i)
        rm[i] = rm[i] - au
        return carry

    loop(2, R - 2, third, 0, UM)
    cx, cy = nx // 2, ny // 2
    sums = add_pairs(jnp.concatenate([pair_rows(rm, tmp, MX, MX, cx, cy), pair_rows(me, tmp2, MX, MX, cx, cy)], axis=0))
    b3 = 0.5 * sums[0:cx * cy].reshape(cx, cy, nz // 2)
    m3 = 0.125 * sums[cx * cy:].reshape(cx, cy, nz // 2)
    both = jnp.concatenate([b3, m3], axis=1)

    def put(k, carry):
        out[k] = both
        return carry

    lax.fori_loop(0, out.shape[0], put, 0)


def finish(got, xm, rm, kx2, ky2, kyp2, kz2, kzp2, dg2, w2, x1, r1, gxl, gxh, gyl, gyh,
           kx, ky, kyp, kz, kzp, dg, w, new,
           bc, mc, wc, pc, sc, ec, mzn, mzp, t1, vm, um, t2, t3, vf, uf, qf, of, sems):
    X, Y, Z = of.shape
    nx, ny, nz = X // 2, Y // 2, Z // 2
    cx, cy, cz = nx // 2, ny // 2, nz // 2
    CX, CY = bc.shape[0], bc.shape[1]
    NX, NY = CX // cx, CY // cy
    px, py = lax.axis_index("gx"), lax.axis_index("gy")

    def place(k, carry):
        gx = lax.rem(px + k + NX - 1, NX)
        for l in range(NY):
            gy = lax.rem(py + l + NY - 1, NY)
            part = got[gx * NY + gy]
            bc[pl.ds(k * cx, cx), l * cy:(l + 1) * cy, :] = part[:, 0:cy, :]
            mc[pl.ds(k * cx, cx), l * cy:(l + 1) * cy, :] = part[:, cy:2 * cy, :]
        return carry

    lax.fori_loop(0, NX, place, 0)
    shift = 16.0 * SHIFT

    def plane(f, zs):
        c1 = zs + (nxt(f, 0) + prv(f, 0))
        c2 = nxt(zs, 0) + prv(zs, 0)
        return 0.5 * c1 + 0.125 * c2, 0.5 * f + 0.125 * c1 + 0.0625 * c2

    def up(i):
        return lax.rem(i + 1, CX)

    def down(i):
        return lax.rem(i + CX - 1, CX)

    def diag_planes(i, carry):
        m = mc[i]
        mn, mp = nxt(m, 1), prv(m, 1)
        mzn[i] = mn
        mzp[i] = mp
        a, o = plane(m, mn + mp)
        sc[i] = a
        pc[i] = o
        return carry

    loop(0, CX, diag_planes, 0, UC)

    def diag_rows(i, carry):
        ms = sc[i] + (pc[up(i)] + pc[down(i)])
        d = shift + 0.5 * (WEIGHT_TOTAL * mc[i] + ms)
        wi = JACOBI / d
        wc[i] = wi
        ec[i] = wi * bc[i]
        return carry

    loop(0, CX, diag_rows, 0, UC)

    def sweep(_, carry):
        def planes(i, c):
            e = ec[i]
            en, ep = nxt(e, 1), prv(e, 1)
            a, o = plane(e, en + ep)
            am, om = plane(mc[i] * e, mzn[i] * en + mzp[i] * ep)
            sc[i] = a
            pc[i] = o
            t1[i] = am
            t1[CX + i] = om
            return c

        loop(0, CX, planes, 0, UC)

        def rows(i, c):
            se = sc[i] + (pc[up(i)] + pc[down(i)])
            sm = t1[i] + (t1[CX + up(i)] + t1[CX + down(i)])
            e = ec[i]
            ec[i] = e + (wc[i] * (bc[i] + 0.5 * (mc[i] * se + sm)) - JACOBI * e)
            return c

        return loop(0, CX, rows, carry, UC)

    lax.fori_loop(0, SWEEPS - 1, sweep, 0)
    zero = jnp.zeros((CY, cz), F32)

    def total(i, c):
        return c[0] + bc[i], c[1] + ec[i], c[2] + mc[i]

    sb, se, sm = loop(0, CX, total, (zero, zero, zero), UC)
    scale = 1.0 / (CX * CY * cz)
    mean_b = jnp.sum(jnp.sum(sb, axis=0, keepdims=True), axis=1, keepdims=True) * scale
    mean_e = jnp.sum(jnp.sum(se, axis=0, keepdims=True), axis=1, keepdims=True) * scale
    mean_m = jnp.sum(jnp.sum(sm, axis=0, keepdims=True), axis=1, keepdims=True) * scale
    kappa = JACOBI * (mean_b - shift * mean_e) / (shift + WEIGHT_TOTAL * mean_m)

    ex, ey = cx + 4, cy + 4
    e = ec[cx - 2:cx - 2 + ex] + kappa.reshape(1, 1, 1)
    ed = double(e.reshape(ex * CY, cz)).reshape(ex, CY, nz)[:, cy - 2:cy - 2 + ey, :]
    for a in range(ex):
        both = repeat_rows(t2, ed[a])
        vm[2 * a] = both
        vm[2 * a + 1] = both
    R = nx + 2 * MX
    co2 = (kx2, ky2, kyp2, kz2, kzp2, dg2, w2)
    co = (kx, ky, kyp, kz, kzp, dg, w)

    def mid_first(i, carry):
        au, c = apply_row(vm, co2, i)
        res = rm[i] - au
        upd = (w2[i] * res) * INV_C
        rm[i] = res
        um[i] = upd
        xm[i] = xm[i] + c + upd
        return carry

    loop(2, R - 2, mid_first, 0, UM)

    def mid_second(i, carry):
        au, c = apply_row(um, co2, i)
        xm[i] = xm[i] + (ALPHA * c + BETA * (w2[i] * (rm[i] - au)))
        return carry

    loop(3, R - 3, mid_second, 0, UM)

    ye = Y + 2 * FY
    wide = nx + 2
    big = double(xm[MX - 1:MX - 1 + wide].reshape(wide * (ny + 2 * MX), nz))
    big = big.reshape(wide, ny + 2 * MX, Z)[:, MX - 2:MX - 2 + ny + 4, :]
    for a in range(wide):
        both = repeat_rows(t3, big[a])
        vf[1 + 2 * a] = both
        vf[2 + 2 * a] = both
    RF = X + 2 * FX
    uf[...] = r1[...]
    for row, msg in ((FX - 1, gxl), (FX + X, gxh)):
        for g in range(2):
            uf[row, FY:FY + Y, g * nz:(g + 1) * nz] = msg[8 + g]
    for colj, msg in ((FY - 1, gyl), (FY + Y, gyh)):
        for h in range(2):
            for k in range(ny):
                for g in range(2):
                    uf[FX + h * ny + k, colj:colj + 1, g * nz:(g + 1) * nz] = msg[nx + 2 * h + g, k:k + 1, :]

    def fine_first(i, carry):
        au, _ = apply_row(vf, co, i)
        res = uf[i] - au
        uf[i] = res
        qf[i] = (w[i] * res) * INV_C
        return carry

    loop(2, RF - 2, fine_first, 0, UF)

    def fine_second(i, carry):
        au, c = apply_row(qf, co, i)
        upd = vf[i] + ((1.0 + ALPHA) * c + BETA * (w[i] * (uf[i] - au)))
        of[i - FX] = (x1[i] + upd)[FY:FY + Y]
        return carry

    part = X // PIECES
    copies = []
    for k in range(PIECES):
        lo = k * part
        loop(FX + lo, FX + lo + part, fine_second, 0, UF)
        src = of.at[pl.ds(lo, part)]
        copies.append(pltpu.make_async_copy(src, new.at[pl.ds(lo, part)], sems.at[k]))
        copies[-1].start()
    for copy in copies:
        copy.wait()


def vmem_call(body, name, out_shape, scratch, inputs, hbm_in=0, hbm_out=False):
    space = pl.BlockSpec(memory_space=pltpu.VMEM)
    far = pl.BlockSpec(memory_space=pltpu.HBM)
    single = not isinstance(out_shape, (list, tuple))
    return pl.pallas_call(
        body,
        name=name,
        out_shape=out_shape,
        in_specs=[far] * hbm_in + [space] * (len(inputs) - hbm_in),
        out_specs=(far if hbm_out else space) if single else [space] * len(out_shape),
        scratch_shapes=scratch,
        compiler_params=pltpu.CompilerParams(vmem_limit_bytes=VMEM_LIMIT),
    )(*inputs)


X_DIRS = ((1, 0), (-1, 0))
Y_DIRS = ((0, 1), (0, -1))
CORNERS = ((1, 1), (1, -1), (-1, 1), (-1, -1))


def exchange(messages, dirs):
    nx, ny = lax.axis_size("gx"), lax.axis_size("gy")
    got = []
    for msg, (dx, dy) in zip(messages, dirs):
        pairs = [(i * ny + j, ((i + dx) % nx) * ny + (j + dy) % ny) for i in range(nx) for j in range(ny)]
        got.append(lax.ppermute(msg, ("gx", "gy"), pairs))
    return got


def sd(*shape):
    return jax.ShapeDtypeStruct(shape, F32)


def vm(*shape):
    return pltpu.VMEM(shape, F32)


def local(pressure, divergence, inverse_density):
    X, Y, Z = pressure.shape
    nx, ny, nz = X // 2, Y // 2, Z // 2
    cx, cy, cz = nx // 2, ny // 2, nz // 2
    NX, NY = lax.axis_size("gx"), lax.axis_size("gy")
    xe, ye = X + 2 * FX, Y + 2 * FY
    mxe, mye = nx + 2 * MX, ny + 2 * MX
    fine = tuple(pltpu.with_memory_space_constraint(a, pltpu.HBM) for a in (pressure, divergence, inverse_density))
    msgs = vmem_call(pack_fine, "pack_fine",
                     [sd(X, Y, Z)] * 3 + [sd(X, 8, Z)] * 2 + [sd(8, Y, Z)] * 2 + [sd(2, 8, Z)] * 4,
                     [pltpu.SemaphoreType.DMA((3 * PIECES,))], fine, hbm_in=3)
    got = exchange(msgs[3:], Y_DIRS + X_DIRS + CORNERS)
    res = vmem_call(
        smooth_fine, "smooth_fine",
        [sd(xe, ye, Z)] * 9 + [sd(nx, ny, nz)] * 2
        + [sd(12, ny, nz)] * 2 + [sd(nx + 5, 8, nz)] * 2,
        [vm(xe, ye, Z)] * 3 + [vm(nx, Z // LANES, ye, LANES), vm(nx + 2, Z // LANES, ye, LANES)],
        tuple(msgs[:3]) + tuple(got))
    x1, r1 = res[:2]
    fine_co = tuple(res[2:9])
    b2, m2 = res[9:11]
    cols = exchange(res[13:15], Y_DIRS)
    rows = exchange(vmem_call(spread_rows, "spread_rows", [sd(10, mye, nz)] * 2, [],
                              (*cols, *res[11:13])), X_DIRS)
    got2 = rows + cols
    *mid, out = vmem_call(
        smooth_mid, "smooth_mid",
        [sd(mxe, mye, nz)] * 9 + [sd(NX * NY, cx, 2 * cy, cz)],
        [vm(mxe, mye, nz)] * 3 + [vm(cx, nz // LANES, mye, LANES)] * 2,
        (b2, m2) + tuple(got2))
    gathered = lax.all_to_all(out, ("gx", "gy"), 0, 0)
    CX, CY = NX * cx, NY * cy
    return vmem_call(
        finish, "finish", sd(X, Y, Z),
        [vm(CX, CY, cz)] * 8 + [vm(2 * CX, CY, cz)] + [vm(mxe, mye, nz)] * 2 + [vm(nz // LANES, mye, LANES), vm(Z // LANES, ye, LANES)] + [vm(xe, ye, Z)] * 3
        + [vm(X, Y, Z), pltpu.SemaphoreType.DMA((PIECES,))],
        (gathered, *mid, x1, r1) + tuple(got2) + fine_co, hbm_out=True)


def solution(mesh):
    return jax.shard_map(
        local,
        mesh=mesh,
        in_specs=(P("gx", "gy", None),) * 3,
        out_specs=P("gx", "gy", None),
        check_vma=False,
    )
```

```python
import jax
import jax.numpy as jnp
from jax import lax
from jax.experimental import pallas as pl
from jax.experimental.pallas import tpu as pltpu
from jax.sharding import PartitionSpec as P

SWEEPS = 4
SHIFT = 0.05
CENTER = (2.0 + 0.3) / 2
HALF = (2.0 - 0.3) / 2
Q0 = CENTER / HALF
P0 = 1.0 / Q0
P1 = 1.0 / (2.0 * Q0 - P0)
ALPHA = P1 * P0
BETA = 2.0 * P1 / HALF
INV_C = 1.0 / CENTER
JACOBI = 0.8
WEIGHT_TOTAL = 5.0

FX = 3
FY = 4
MX = 4

F32 = jnp.float32
UF = 4
UM = 7
UC = 8
PIECES = 4
VMEM_LIMIT = 20 * 1024 * 1024


def nxt(v, axis):
    return pltpu.roll(v, v.shape[axis] - 1, axis)


def prv(v, axis):
    return pltpu.roll(v, 1, axis)


def loop(low, high, body, init, unroll):
    rest = (high - low) % unroll
    carry = init
    for k in range(rest):
        carry = body(low + k, carry)
    start = low + rest

    def group(g, c):
        for k in range(unroll):
            c = body(start + g * unroll + k, c)
        return c

    return lax.fori_loop(0, (high - start) // unroll, group, carry)


def coefficients(m_ref, k, rows, shift, unroll):
    kx, ky, kyp, kz, kzp, d_ref, w_ref = k
    kx[0] = 0.5 * (m_ref[0] + m_ref[1])

    def body(i, carry):
        m = m_ref[i]
        fx = 0.5 * (m + m_ref[i + 1])
        fxp = 0.5 * (m + m_ref[i - 1])
        fz = 0.5 * (m + nxt(m, 1))
        fzp = 0.5 * (m + prv(m, 1))
        fy = 0.5 * (m + nxt(m, 0))
        fyp = 0.5 * (m + prv(m, 0))
        kx[i] = fx
        ky[i] = fy
        kyp[i] = fyp
        kz[i] = fz
        kzp[i] = fzp
        d = shift + ((fx + fxp) + (fy + fyp) + (fz + fzp))
        d_ref[i] = d
        w_ref[i] = 1.0 / d
        return carry

    loop(1, rows - 1, body, 0, unroll)


def apply_row(v_ref, k, i):
    kx, ky, kyp, kz, kzp, d_ref, w_ref = k
    c = v_ref[i]
    z = kz[i] * nxt(c, 1) + kzp[i] * prv(c, 1)
    y = ky[i] * nxt(c, 0) + kyp[i] * prv(c, 0)
    x = kx[i] * v_ref[i + 1] + kx[i - 1] * v_ref[i - 1]
    return d_ref[i] * c - ((x + y) + z), c


BF16 = jnp.bfloat16


def select(a, table):
    hi = a.astype(BF16)
    rest = a - hi.astype(F32)
    mid = rest.astype(BF16)
    low = (rest - mid.astype(F32)).astype(BF16)
    n = a.shape[0]
    out = jnp.dot(jnp.concatenate([hi, mid, low], axis=0), table, preferred_element_type=F32)
    return (out[0:n] + out[n:2 * n]) + out[2 * n:3 * n]


def chunks_as_rows(a, width):
    return jnp.concatenate([a[:, g * width:(g + 1) * width] for g in range(a.shape[1] // width)], axis=0)


def rows_as_chunks(a, count):
    n = a.shape[0] // count
    return jnp.concatenate([a[g * n:(g + 1) * n] for g in range(count)], axis=1)


def add_pairs(a):
    row = lax.broadcasted_iota(jnp.int32, (2 * LANES, LANES), 0)
    col = lax.broadcasted_iota(jnp.int32, (2 * LANES, LANES), 1)
    table = jnp.where(row // 2 == col, 1.0, 0.0).astype(BF16)
    return rows_as_chunks(select(chunks_as_rows(a, 2 * LANES), table), a.shape[1] // (2 * LANES))


def double(a):
    row = lax.broadcasted_iota(jnp.int32, (LANES, 2 * LANES), 0)
    col = lax.broadcasted_iota(jnp.int32, (LANES, 2 * LANES), 1)
    table = jnp.where(col // 2 == row, 1.0, 0.0).astype(BF16)
    return rows_as_chunks(select(chunks_as_rows(a, LANES), table), a.shape[1] // LANES)


LANES = 128


def put_lanes(tmp, a, val):
    for g in range(val.shape[1] // LANES):
        tmp[a, g] = val[:, g * LANES:(g + 1) * LANES]


def take_pairs(tmp, a, y0, ny, chunks):
    parts = [tmp[a, g, pl.ds(y0, ny, stride=2), :] + tmp[a, g, pl.ds(y0 + 1, ny, stride=2), :] for g in range(chunks)]
    return jnp.concatenate(parts, axis=1)


def repeat_rows(tmp, val):
    n, chunks = val.shape[0], val.shape[1] // LANES
    for g in range(chunks):
        part = val[:, g * LANES:(g + 1) * LANES]
        tmp[g, pl.ds(0, n, stride=2), :] = part
        tmp[g, pl.ds(1, n, stride=2), :] = part
    return jnp.concatenate([tmp[g] for g in range(chunks)], axis=1)


def pair_rows(ref, tmp, x0, y0, nx, ny):
    z = ref.shape[2]
    for a in range(nx):
        put_lanes(tmp, a, ref[x0 + 2 * a] + ref[x0 + 2 * a + 1])
    return jnp.concatenate([take_pairs(tmp, a, y0, ny, z // LANES) for a in range(nx)], axis=0)


def put_tiles(out, at, rows):
    n = rows.shape[1] // 8
    for k in range(rows.shape[0]):
        for t in range(n):
            out[(at + k) * n + t] = rows[k, 8 * t:8 * t + 8]


def pack_fine(x_in, b_in, m_in, x, b, m, m3, *outs):
    X, Y = x.shape[0], x.shape[1]
    *outs, tmp, sems = outs
    cx, cy, cz = m3.shape
    copies = []
    for src, dst in ((x_in, x), (b_in, b), (m_in, m)):
        for k in range(PIECES):
            part = pl.ds(k * (X // PIECES), X // PIECES)
            copies.append(pltpu.make_async_copy(src.at[part], dst.at[part], sems.at[len(copies)]))
    for copy in copies:
        copy.start()
    for copy in copies:
        copy.wait()
    gyp, gym, gxp, gxm, cpp, cpm, cmp_, cmm = outs
    for a in range(cx):
        put_lanes(tmp, a, (m[4 * a] + m[4 * a + 1]) + (m[4 * a + 2] + m[4 * a + 3]))
    chunks = tmp.shape[1]
    quads = [jnp.concatenate([(tmp[a, g, pl.ds(0, cy, stride=4), :] + tmp[a, g, pl.ds(1, cy, stride=4), :])
                              + (tmp[a, g, pl.ds(2, cy, stride=4), :] + tmp[a, g, pl.ds(3, cy, stride=4), :])
                              for g in range(chunks)], axis=1) for a in range(cx)]
    coarse = add_pairs(add_pairs(jnp.concatenate(quads, axis=0))) * (1.0 / 64.0)
    m3[...] = coarse.reshape(cx, cy, cz)
    half = cx * cy // 2
    for out in (gyp, gym, gxp, gxm):
        last = out.shape[0] - 1
        out[last, 0:half, 0:cz] = coarse[0:half]
        out[last, 0:half, cz:2 * cz] = coarse[half:2 * half]
    for out in (cpp, cpm, cmp_, cmm):
        for a in range(cx):
            for l in range(cy):
                out[a // 2, 6 + a % 2:7 + a % 2, l * cz:(l + 1) * cz] = coarse[a * cy + l:a * cy + l + 1]
    for out, sl in ((gxp, lambda k: slice(X - k, X)), (gxm, lambda k: slice(0, k))):
        put_tiles(out, 0, x[sl(3)])
        put_tiles(out, 3, b[sl(2)])
        put_tiles(out, 5, m[sl(3)])
    for out, sl in ((gyp, lambda k: slice(Y - k, Y)), (gym, lambda k: slice(0, k))):
        out[0:X, 0:3, :] = x[:, sl(3), :]
        out[0:X, 3:5, :] = b[:, sl(2), :]
        out[0:X, 5:8, :] = m[:, sl(3), :]
    for out, sx, sy in ((cpp, 1, 1), (cpm, 1, -1), (cmp_, -1, 1), (cmm, -1, -1)):
        rows = slice(X - 2, X) if sx > 0 else slice(0, 2)
        cols = slice(Y - 2, Y) if sy > 0 else slice(0, 2)
        out[:, 0:2, :] = x[rows, cols, :]
        out[:, 2:4, :] = b[rows, cols, :]
        out[:, 4:6, :] = m[rows, cols, :]


def smooth_fine(x, b, m, m3, gyl, gyh, gxl, gxh, cll, clh, chl, chh,
                xe, r, kx, ky, kyp, kz, kzp, dg, w, b2, m2, m9, sxp, sxm, syp, sym,
                be, me, u, tmp, tmp2):
    X, Y, Z = x.shape
    R = X + 2 * FX
    x_end, y_end = FX + X, FY + Y
    for ext, own, lo, n in ((xe, x, 0, 3), (be, b, 3, 2), (me, m, 5, 3)):
        ext[FX:x_end, FY:y_end, :] = own[...]
        for msg, r0 in ((gxl, FX - n), (gxh, x_end)):
            for k in range(n):
                for t in range(Y // 8):
                    ext[r0 + k, FY + 8 * t:FY + 8 * t + 8, :] = msg[(lo + k) * (Y // 8) + t]
        ext[FX:x_end, FY - n:FY, :] = gyl[0:X, lo:lo + n, :]
        ext[FX:x_end, y_end:y_end + n, :] = gyh[0:X, lo:lo + n, :]
    for msg, rows, cols in ((cll, slice(FX - 2, FX), slice(FY - 2, FY)),
                            (clh, slice(FX - 2, FX), slice(y_end, y_end + 2)),
                            (chl, slice(x_end, x_end + 2), slice(FY - 2, FY)),
                            (chh, slice(x_end, x_end + 2), slice(y_end, y_end + 2))):
        xe[rows, cols, :] = msg[:, 0:2, :]
        be[rows, cols, :] = msg[:, 2:4, :]
        me[rows, cols, :] = msg[:, 4:6, :]
    co = (kx, ky, kyp, kz, kzp, dg, w)
    coefficients(me, co, R, SHIFT, UF)

    def first(i, carry):
        ax, _ = apply_row(xe, co, i)
        res = be[i] - ax
        r[i] = res
        u[i] = (w[i] * res) * INV_C
        return carry

    loop(1, R - 1, first, 0, UF)

    def second(i, carry):
        au, c = apply_row(u, co, i)
        res = r[i] - au
        r[i] = res
        up = ALPHA * c + BETA * (w[i] * res)
        xe[i] = xe[i] + c + up
        be[i] = up
        return carry

    loop(2, R - 2, second, 0, UF)

    def third(i, carry):
        au, _ = apply_row(be, co, i)
        r[i] = r[i] - au
        return carry

    loop(3, R - 3, third, 0, UF)
    nx, ny, nz = X // 2, Y // 2, Z // 2
    sums = jnp.concatenate([pair_rows(r, tmp, FX, FY, nx, ny), pair_rows(me, tmp2, FX - 2, 0, nx + 2, ny + 4)], axis=0)
    sums = add_pairs(sums)
    b2[...] = 0.5 * sums[0:nx * ny].reshape(nx, ny, nz)
    mm = 0.125 * sums[nx * ny:].reshape(nx + 2, ny + 4, nz)
    cells = mm[1:nx + 1, 2:2 + ny, :]
    m2[...] = cells
    fz = 0.5 * (cells + nxt(cells, 2))
    fzp = prv(fz, 2)
    diag = (4.0 * SHIFT + 0.5 * (4.0 * cells + mm[0:nx, 2:2 + ny, :] + mm[2:nx + 2, 2:2 + ny, :]
                                 + mm[1:nx + 1, 1:1 + ny, :] + mm[1:nx + 1, 3:3 + ny, :]) + (fz + fzp))
    u2 = (b2[...] * (1.0 / diag)) * INV_C
    bb = b2[...]
    sxp[0:1] = u2[nx - 4:nx - 3]
    sxp[1:4] = bb[nx - 3:nx]
    sxp[4:8] = cells[nx - 4:nx]
    sxm[0:3] = bb[0:3]
    sxm[3:4] = u2[3:4]
    sxm[4:8] = cells[0:4]
    syp[0:nx, 0:1, :] = u2[:, ny - 4:ny - 3, :]
    syp[0:nx, 1:4, :] = bb[:, ny - 3:ny, :]
    syp[0:nx, 4:8, :] = cells[:, ny - 4:ny, :]
    sym[0:nx, 0:3, :] = bb[:, 0:3, :]
    sym[0:nx, 3:4, :] = u2[:, 3:4, :]
    sym[0:nx, 4:8, :] = cells[:, 0:4, :]
    for dst, src in ((sxp, r[FX + X - 1, FY:y_end]), (sxm, r[FX, FY:y_end])):
        for h in range(2):
            for g in range(2):
                dst[8 + 2 * h + g] = src[h * ny:(h + 1) * ny, g * nz:(g + 1) * nz]
    for dst, j in ((syp, Y - 1), (sym, 0)):
        for h in range(2):
            for k in range(ny):
                row = r[FX + h * ny + k, FY + j:FY + j + 1, :]
                for g in range(2):
                    dst[nx + 2 * h + g, k:k + 1, :] = row[:, g * nz:(g + 1) * nz]
    for out, j0, step in ((syp, ny - 1, -1), (sym, 0, 1)):
        for t in range(3):
            j = j0 + step * t
            out[nx + 4, t:t + 1, :] = u2[nx - 4 + t, j:j + 1, :]
            out[nx + 4, 3 + t:4 + t, :] = u2[3 - t, j:j + 1, :]
    cx, cy, cz = m3.shape
    half = cx * cy // 2
    m9[:, 3 * cy:4 * cy, :] = jnp.ones((3 * cx, cy, cz), F32)
    m9[cx:2 * cx, cy:2 * cy, :] = m3[...]
    for msg, c0 in ((gyl, 0), (gyh, 2 * cy)):
        both = jnp.concatenate([msg[X, 0:half, 0:cz], msg[X, 0:half, cz:2 * cz]], axis=0)
        m9[cx:2 * cx, c0:c0 + cy, :] = both.reshape(cx, cy, cz)
    for msg, r0 in ((gxl, 0), (gxh, 2 * cx)):
        both = jnp.concatenate([msg[Y, 0:half, 0:cz], msg[Y, 0:half, cz:2 * cz]], axis=0)
        m9[r0:r0 + cx, cy:2 * cy, :] = both.reshape(cx, cy, cz)
    for msg, r0, c0 in ((cll, 0, 0), (clh, 0, 2 * cy), (chl, 2 * cx, 0), (chh, 2 * cx, 2 * cy)):
        for a in range(cx):
            for l in range(cy):
                m9[r0 + a, c0 + l:c0 + l + 1, :] = msg[a // 2, 6 + a % 2:7 + a % 2, l * cz:(l + 1) * cz]
    for out, line in ((syp, cy - 1), (sym, 2 * cy)):
        for k in range(3 * cx):
            out[nx + 5, k % ny:k % ny + 1, (k // ny) * cz:(k // ny + 1) * cz] = m9[k, line:line + 1, :]


def far_lines(row, k, gyl, gyh):
    cz, ny = row.shape[1], gyl.shape[1]
    nx = gyl.shape[0] - 6
    col = lax.broadcasted_iota(jnp.int32, row.shape, 0)
    pick = lambda msg: msg[nx + 5, k % ny:k % ny + 1, (k // ny) * cz:(k // ny + 1) * cz]
    row = jnp.where(col == 3 * row.shape[0] // 4, pick(gyh), row)
    return jnp.where(col == row.shape[0] - 1, pick(gyl), row)


def spread_rows(gyl, gyh, sxp, sxm, m9, axp, axm):
    ny, nx = sxp.shape[1], gyl.shape[0] - 6
    cx, cz = m9.shape[0] // 3, m9.shape[2]
    for out, k in ((axp, cx - 1), (axm, 2 * cx)):
        out[10, :, 0:cz] = far_lines(m9[k], k, gyl, gyh)
    yend = MX + ny
    for own, out, r0, line in ((sxp, axp, nx - 4, 0), (sxm, axm, 0, 3)):
        for lo in (0, 4):
            out[lo:lo + 4, MX:yend, :] = own[lo:lo + 4]
            out[lo:lo + 4, 0:MX, :] = gyl[r0:r0 + 4, lo:lo + 4, :]
            out[lo:lo + 4, yend:yend + MX, :] = gyh[r0:r0 + 4, lo:lo + 4, :]
        for t in range(3):
            row = t if line == 0 else 3 - t
            out[row, 3 - t:4 - t, :] = gyl[nx + 4, line + t:line + t + 1, :]
            out[row, yend + t:yend + t + 1, :] = gyh[nx + 4, line + t:line + t + 1, :]
        for h in range(2):
            for g in range(2):
                out[8 + g, h * ny:(h + 1) * ny, :] = own[8 + 2 * h + g]


def smooth_mid(b2, m2, m3, test, w3, gxl, gxh, gyl, gyh,
               xm, rm, kx, ky, kyp, kz, kzp, dg, w, out,
               qe, me, u, tmp):
    nx, ny, nz = b2.shape
    R = nx + 2 * MX
    shift = 4.0 * SHIFT
    xend, yend = MX + nx, MX + ny
    for ext, own, lo in ((qe, b2, 0), (me, m2, 4)):
        ext[MX:xend, MX:yend, :] = own[...]
        ext[MX:xend, 0:MX, :] = gyl[0:nx, lo:lo + 4, :]
        ext[MX:xend, yend:yend + MX, :] = gyh[0:nx, lo:lo + 4, :]
        ext[0:MX] = gxl[lo:lo + 4]
        ext[xend:xend + MX] = gxh[lo:lo + 4]
    co = (kx, ky, kyp, kz, kzp, dg, w)
    coefficients(me, co, R, shift, UM)
    col = lax.broadcasted_iota(jnp.int32, (ny + 2 * MX, nz), 0)
    dcol = jnp.maximum(jnp.maximum(MX - col, col - (yend - 1)), 0)

    def first(i, carry):
        di = jnp.maximum(jnp.maximum(MX - i, i - (xend - 1)), 0)
        q = qe[i]
        sent = (dcol + di == 5) | (dcol == 4) | (di == 4)
        u[i] = jnp.where(sent, q, (w[i] * q) * INV_C)
        return carry

    u[0] = qe[0]
    u[R - 1] = qe[R - 1]
    loop(1, R - 1, first, 0, UM)

    def second(i, carry):
        au, c = apply_row(u, co, i)
        res = qe[i] - au
        rm[i] = res
        up = ALPHA * c + BETA * (w[i] * res)
        xm[i] = c + up
        qe[i] = up
        return carry

    loop(1, R - 1, second, 0, UM)

    def third(i, carry):
        au, _ = apply_row(qe, co, i)
        rm[i] = rm[i] - au
        return carry

    loop(2, R - 2, third, 0, UM)
    cx, cy = nx // 2, ny // 2
    b3 = 0.5 * add_pairs(pair_rows(rm, tmp, MX, MX, cx, cy)).reshape(cx, cy, nz // 2)
    kept = jnp.sum(test[...] * b3, axis=0)
    mass = jnp.sum(m3[...], axis=0)
    h = cy // 2
    extra = jnp.concatenate([kept[0:h] + kept[h:cy], mass[0:h] + mass[h:cy]], axis=0)
    both = jnp.concatenate([w3[...] * b3, extra.reshape(1, cy, nz // 2)], axis=0)

    def put(k, carry):
        out[k] = both
        return carry

    lax.fori_loop(0, out.shape[0], put, 0)


def plane(f, zs):
    c1 = zs + (nxt(f, 0) + prv(f, 0))
    c2 = nxt(zs, 0) + prv(zs, 0)
    return 0.5 * c1 + 0.125 * c2, 0.5 * f + 0.125 * c1 + 0.0625 * c2


def weighted_sums(f, m, mzn, mzp, lo, hi):
    own, out = {}, {}
    for i in range(lo - 1, hi + 1):
        fn, fp = nxt(f[i], 1), prv(f[i], 1)
        a, o = plane(f[i], fn + fp)
        am, om = plane(m[i] * f[i], mzn[i] * fn + mzp[i] * fp)
        own[i], out[i] = (a, am), (o, om)
    return {i: m[i] * (own[i][0] + (out[i - 1][0] + out[i + 1][0])) + (own[i][1] + (out[i - 1][1] + out[i + 1][1]))
            for i in range(lo, hi)}


def rotate_rows(m, rows, mzn, mzp):
    for i in range(rows):
        mzn[i] = nxt(m[i], 1)
        mzp[i] = prv(m[i], 1)


def inverse_rows(m, mzn, mzp, lo, hi):
    planes = {i: plane(m[i], mzn[i] + mzp[i]) for i in range(lo - 1, hi + 1)}
    return {i: JACOBI / (16.0 * SHIFT + 0.5 * (WEIGHT_TOTAL * m[i] + (planes[i][0] + (planes[i - 1][1] + planes[i + 1][1]))))
            for i in range(lo, hi)}


def mean_weights(m9, test, w3, mzn, mzp):
    rows, (cx, cy, cz) = m9.shape[0], test.shape
    rotate_rows(m9, rows, mzn, mzp)
    w = inverse_rows(m9, mzn, mzp, 1, rows - 1)
    one = jnp.ones(m9.shape[1:], F32)
    g = {i: one for i in range(1, rows - 1)}
    total = {i: one for i in range(cx, 2 * cx)}
    for sweep in range(SWEEPS - 1):
        lo, hi = 2 + sweep, rows - 2 - sweep
        sums = weighted_sums({i: w[i] * g[i] for i in range(lo - 1, hi + 1)}, m9, mzn, mzp, lo, hi)
        g = {i: (1.0 - JACOBI) * g[i] + 0.5 * sums[i] for i in range(lo, hi)}
        total = {i: total[i] + g[i] for i in total}
    for i in range(cx):
        wi = w[cx + i]
        test[i] = (1.0 - 16.0 * SHIFT * (wi * total[cx + i]))[cy:2 * cy]
        w3[i] = wi[cy:2 * cy]


def coarse_weights(m9, gyl, gyh, gxl, gxh, mw, mzn, mzp, wc):
    rows, cz = mw.shape[0], mw.shape[2]
    mw[0] = gxl[10, :, 0:cz]
    mw[rows - 1] = gxh[10, :, 0:cz]
    for k in range(rows - 2):
        mw[1 + k] = far_lines(m9[k], k, gyl, gyh)
    rotate_rows(mw, rows, mzn, mzp)
    w = inverse_rows(mw, mzn, mzp, 1, rows - 1)
    for i in w:
        wc[i] = w[i]


def finish(got, m9, xm, rm, kx2, ky2, kyp2, kz2, kzp2, dg2, w2, x1, r1, gxl, gxh, gyl, gyh,
           kx, ky, kyp, kz, kzp, dg, w, new,
           ec, mw, mzn, mzp, wc, vm, um, t2, t3, vf, uf, qf, of, sems):
    X, Y, Z = of.shape
    nx, ny, nz = X // 2, Y // 2, Z // 2
    cx, cy, cz = nx // 2, ny // 2, nz // 2
    NX, NY = lax.axis_size("gx"), lax.axis_size("gy")
    px, py = lax.axis_index("gx"), lax.axis_index("gy")
    CY = ec.shape[1]
    rows = 3 * cx + 2
    coarse_weights(m9, gyl, gyh, gxl, gxh, mw, mzn, mzp, wc)

    for k in range(-2, 3):
        gx = lax.rem(px + k + NX, NX) * NY
        take = slice(cx - 1, cx) if k == -2 else slice(0, 1) if k == 2 else slice(0, cx)
        r0 = (k + 1) * cx + 1 if k > -2 else 0
        n = take.stop - take.start
        for l in range(-2, 3):
            part = got[gx + lax.rem(py + l + NY, NY)][take]
            if l == -2:
                ec[r0:r0 + n, CY - 1:CY, :] = part[:, cy - 1:cy, :]
            elif l == 2:
                ec[r0:r0 + n, 3 * cy:CY - 1, :] = part[:, 0:cy - 1, :]
            else:
                ec[r0:r0 + n, (l + 1) * cy:(l + 2) * cy, :] = part[:, 0:cy, :]
    e = {i: ec[i] for i in range(rows)}
    for sweep in range(SWEEPS - 1):
        lo, hi = 1 + sweep, rows - 1 - sweep
        sums = weighted_sums(e, mw, mzn, mzp, lo, hi)
        e = {i: (1.0 - JACOBI) * e[i] + (ec[i] + (0.5 * wc[i]) * sums[i]) for i in range(lo, hi)}
    sums = got[0, cx]
    for k in range(1, NX * NY):
        sums = sums + got[k, cx]
    cells = cx * cy * cz * NX * NY
    h = cy // 2
    total = jnp.sum(jnp.sum(sums[0:h], axis=0, keepdims=True), axis=1, keepdims=True) * (1.0 / cells)
    mean_m = jnp.sum(jnp.sum(sums[h:cy], axis=0, keepdims=True), axis=1, keepdims=True) * (1.0 / cells)
    kappa = JACOBI * total / (16.0 * SHIFT + WEIGHT_TOTAL * mean_m)

    ex, ey = cx + 4, cy + 4
    e = jnp.concatenate([e[cx - 1 + i] + kappa for i in range(ex)], axis=0)
    ed = double(e).reshape(ex, CY, nz)[:, cy - 2:cy - 2 + ey, :]
    for a in range(ex):
        both = repeat_rows(t2, ed[a])
        vm[2 * a] = both
        vm[2 * a + 1] = both
    R = nx + 2 * MX
    co2 = (kx2, ky2, kyp2, kz2, kzp2, dg2, w2)
    co = (kx, ky, kyp, kz, kzp, dg, w)

    def mid_first(i, carry):
        au, c = apply_row(vm, co2, i)
        res = rm[i] - au
        upd = (w2[i] * res) * INV_C
        rm[i] = res
        um[i] = upd
        xm[i] = xm[i] + c + upd
        return carry

    loop(2, R - 2, mid_first, 0, UM)

    def mid_second(i, carry):
        au, c = apply_row(um, co2, i)
        xm[i] = xm[i] + (ALPHA * c + BETA * (w2[i] * (rm[i] - au)))
        return carry

    loop(3, R - 3, mid_second, 0, UM)

    ye = Y + 2 * FY
    wide = nx + 2
    big = double(xm[MX - 1:MX - 1 + wide].reshape(wide * (ny + 2 * MX), nz))
    big = big.reshape(wide, ny + 2 * MX, Z)[:, MX - 2:MX - 2 + ny + 4, :]
    for a in range(wide):
        both = repeat_rows(t3, big[a])
        vf[1 + 2 * a] = both
        vf[2 + 2 * a] = both
    RF = X + 2 * FX
    uf[...] = r1[...]
    for row, msg in ((FX - 1, gxl), (FX + X, gxh)):
        for g in range(2):
            uf[row, FY:FY + Y, g * nz:(g + 1) * nz] = msg[8 + g]
    for colj, msg in ((FY - 1, gyl), (FY + Y, gyh)):
        for h in range(2):
            for k in range(ny):
                for g in range(2):
                    uf[FX + h * ny + k, colj:colj + 1, g * nz:(g + 1) * nz] = msg[nx + 2 * h + g, k:k + 1, :]

    def fine_first(i, carry):
        au, _ = apply_row(vf, co, i)
        res = uf[i] - au
        uf[i] = res
        qf[i] = (w[i] * res) * INV_C
        return carry

    loop(2, RF - 2, fine_first, 0, UF)

    def fine_second(i, carry):
        au, c = apply_row(qf, co, i)
        upd = vf[i] + ((1.0 + ALPHA) * c + BETA * (w[i] * (uf[i] - au)))
        of[i - FX] = (x1[i] + upd)[FY:FY + Y]
        return carry

    part = X // PIECES
    copies = []
    for k in range(PIECES):
        lo = k * part
        loop(FX + lo, FX + lo + part, fine_second, 0, UF)
        src = of.at[pl.ds(lo, part)]
        copies.append(pltpu.make_async_copy(src, new.at[pl.ds(lo, part)], sems.at[k]))
        copies[-1].start()
    for copy in copies:
        copy.wait()


def vmem_call(body, name, out_shape, scratch, inputs, hbm_in=0, hbm_out=False):
    space = pl.BlockSpec(memory_space=pltpu.VMEM)
    far = pl.BlockSpec(memory_space=pltpu.HBM)
    single = not isinstance(out_shape, (list, tuple))
    return pl.pallas_call(
        body,
        name=name,
        out_shape=out_shape,
        in_specs=[far] * hbm_in + [space] * (len(inputs) - hbm_in),
        out_specs=(far if hbm_out else space) if single else [space] * len(out_shape),
        scratch_shapes=scratch,
        compiler_params=pltpu.CompilerParams(vmem_limit_bytes=VMEM_LIMIT),
    )(*inputs)


X_DIRS = ((1, 0), (-1, 0))
Y_DIRS = ((0, 1), (0, -1))
CORNERS = ((1, 1), (1, -1), (-1, 1), (-1, -1))


def exchange(messages, dirs):
    nx, ny = lax.axis_size("gx"), lax.axis_size("gy")
    got = []
    for msg, (dx, dy) in zip(messages, dirs):
        pairs = [(i * ny + j, ((i + dx) % nx) * ny + (j + dy) % ny) for i in range(nx) for j in range(ny)]
        got.append(lax.ppermute(msg, ("gx", "gy"), pairs))
    return got


def sd(*shape):
    return jax.ShapeDtypeStruct(shape, F32)


def vm(*shape):
    return pltpu.VMEM(shape, F32)


def local(pressure, divergence, inverse_density):
    X, Y, Z = pressure.shape
    nx, ny, nz = X // 2, Y // 2, Z // 2
    cx, cy, cz = nx // 2, ny // 2, nz // 2
    NX, NY = lax.axis_size("gx"), lax.axis_size("gy")
    xe, ye = X + 2 * FX, Y + 2 * FY
    mxe, mye = nx + 2 * MX, ny + 2 * MX
    fine = tuple(pltpu.with_memory_space_constraint(a, pltpu.HBM) for a in (pressure, divergence, inverse_density))
    msgs = vmem_call(pack_fine, "pack_fine",
                     [sd(X, Y, Z)] * 3 + [sd(cx, cy, cz)] + [sd(X + 1, 8, Z)] * 2 + [sd(Y + 1, 8, Z)] * 2 + [sd(2, 8, Z)] * 4,
                     [vm(cx, Z // LANES, Y, LANES), pltpu.SemaphoreType.DMA((3 * PIECES,))], fine, hbm_in=3)
    got = exchange(msgs[4:], Y_DIRS + X_DIRS + CORNERS)
    res = vmem_call(
        smooth_fine, "smooth_fine",
        [sd(xe, ye, Z)] * 9 + [sd(nx, ny, nz)] * 2
        + [sd(3 * cx, 4 * cy, cz)] + [sd(12, ny, nz)] * 2 + [sd(nx + 6, 8, nz)] * 2,
        [vm(xe, ye, Z)] * 3 + [vm(nx, Z // LANES, ye, LANES), vm(nx + 2, Z // LANES, ye, LANES)],
        tuple(msgs[:4]) + tuple(got))
    x1, r1 = res[:2]
    fine_co = tuple(res[2:9])
    b2, m2, m9 = res[9:12]
    m3 = msgs[3]
    test, w3 = vmem_call(mean_weights, "mean_weights", [sd(cx, cy, cz)] * 2, [vm(3 * cx, 4 * cy, cz)] * 2, (m9,))
    cols = exchange(res[14:16], Y_DIRS)
    rows = exchange(vmem_call(spread_rows, "spread_rows", [sd(11, mye, nz)] * 2, [],
                              (*cols, *res[12:14], m9)), X_DIRS)
    got2 = rows + cols
    *mid, out = vmem_call(
        smooth_mid, "smooth_mid",
        [sd(mxe, mye, nz)] * 9 + [sd(NX * NY, cx + 1, cy, cz)],
        [vm(mxe, mye, nz)] * 3 + [vm(cx, nz // LANES, mye, LANES)],
        (b2, m2, m3, test, w3) + tuple(got2))
    gathered = lax.all_to_all(out, ("gx", "gy"), 0, 0)
    window = (3 * cx + 2, 4 * cy, cz)
    return vmem_call(
        finish, "finish", sd(X, Y, Z),
        [vm(*window)] * 5 + [vm(mxe, mye, nz)] * 2 + [vm(nz // LANES, mye, LANES), vm(Z // LANES, ye, LANES)]
        + [vm(xe, ye, Z)] * 3 + [vm(X, Y, Z), pltpu.SemaphoreType.DMA((PIECES,))],
        (gathered, m9, *mid, x1, r1) + tuple(got2) + fine_co, hbm_out=True)


def solution(mesh):
    return jax.shard_map(
        local,
        mesh=mesh,
        in_specs=(P("gx", "gy", None),) * 3,
        out_specs=P("gx", "gy", None),
        check_vma=False,
    )
```

```python
import jax
import jax.numpy as jnp
from jax import lax
from jax.experimental import pallas as pl
from jax.experimental.pallas import tpu as pltpu
from jax.sharding import PartitionSpec as P

SWEEPS = 4
SHIFT = 0.05
CENTER = (2.0 + 0.3) / 2
HALF = (2.0 - 0.3) / 2
Q0 = CENTER / HALF
P0 = 1.0 / Q0
P1 = 1.0 / (2.0 * Q0 - P0)
ALPHA = P1 * P0
BETA = 2.0 * P1 / HALF * CENTER
INV_C = 1.0 / CENTER
JACOBI = 0.8
WEIGHT_TOTAL = 5.0

FX = 3
FY = 4
MX = 4

F32 = jnp.float32
UF = 10
UM = 7
UC = 8
PIECES = 4
VMEM_LIMIT = 20 * 1024 * 1024


def nxt(v, axis):
    return pltpu.roll(v, v.shape[axis] - 1, axis)


def prv(v, axis):
    return pltpu.roll(v, 1, axis)


def loop(low, high, body, init, unroll):
    rest = (high - low) % unroll
    carry = init
    for k in range(rest):
        carry = body(low + k, carry)
    start = low + rest

    def group(g, c):
        for k in range(unroll):
            c = body(start + g * unroll + k, c)
        return c

    return lax.fori_loop(0, (high - start) // unroll, group, carry)


def plain(a):
    return a


def halved(a):
    return 0.5 * a


def coefficients(m_ref, k, rows, shift, unroll):
    kx, ky, kyp, kz, kzp, d_ref, w_ref = k
    kx[0] = m_ref[0] + m_ref[1]

    def body(i, carry):
        m = m_ref[i]
        fx = m + m_ref[i + 1]
        fxp = m + m_ref[i - 1]
        fz = m + nxt(m, 1)
        fzp = m + prv(m, 1)
        fy = m + nxt(m, 0)
        fyp = m + prv(m, 0)
        kx[i] = fx
        ky[i] = fy
        kyp[i] = fyp
        kz[i] = fz
        kzp[i] = fzp
        d = shift + ((fx + fxp) + (fy + fyp) + (fz + fzp))
        d_ref[i] = d
        w_ref[i] = INV_C / d
        return carry

    loop(1, rows - 1, body, 0, unroll)


def apply_row(v_ref, k, i):
    kx, ky, kyp, kz, kzp, d_ref, w_ref = k
    c = v_ref[i]
    z = kz[i] * nxt(c, 1) + kzp[i] * prv(c, 1)
    y = ky[i] * nxt(c, 0) + kyp[i] * prv(c, 0)
    x = kx[i] * v_ref[i + 1] + kx[i - 1] * v_ref[i - 1]
    return d_ref[i] * c - ((x + y) + z), c


BF16 = jnp.bfloat16


def select(a, table):
    hi = a.astype(BF16)
    rest = a - hi.astype(F32)
    mid = rest.astype(BF16)
    low = (rest - mid.astype(F32)).astype(BF16)
    n = a.shape[0]
    out = jnp.dot(jnp.concatenate([hi, mid, low], axis=0), table, preferred_element_type=F32)
    return (out[0:n] + out[n:2 * n]) + out[2 * n:3 * n]


def chunks_as_rows(a, width):
    return jnp.concatenate([a[:, g * width:(g + 1) * width] for g in range(a.shape[1] // width)], axis=0)


def rows_as_chunks(a, count):
    n = a.shape[0] // count
    return jnp.concatenate([a[g * n:(g + 1) * n] for g in range(count)], axis=1)


def add_pairs(a):
    row = lax.broadcasted_iota(jnp.int32, (2 * LANES, LANES), 0)
    col = lax.broadcasted_iota(jnp.int32, (2 * LANES, LANES), 1)
    table = jnp.where(row // 2 == col, 1.0, 0.0).astype(BF16)
    return rows_as_chunks(select(chunks_as_rows(a, 2 * LANES), table), a.shape[1] // (2 * LANES))


def double(a):
    row = lax.broadcasted_iota(jnp.int32, (LANES, 2 * LANES), 0)
    col = lax.broadcasted_iota(jnp.int32, (LANES, 2 * LANES), 1)
    table = jnp.where(col // 2 == row, 1.0, 0.0).astype(BF16)
    return rows_as_chunks(select(chunks_as_rows(a, LANES), table), a.shape[1] // LANES)


LANES = 128


def put_lanes(tmp, a, val):
    for g in range(val.shape[1] // LANES):
        tmp[a, g] = val[:, g * LANES:(g + 1) * LANES]


def take_pairs(tmp, a, y0, ny, chunks):
    parts = [tmp[a, g, pl.ds(y0, ny, stride=2), :] + tmp[a, g, pl.ds(y0 + 1, ny, stride=2), :] for g in range(chunks)]
    return jnp.concatenate(parts, axis=1)


def repeat_rows(tmp, val):
    n, chunks = val.shape[0], val.shape[1] // LANES
    for g in range(chunks):
        part = val[:, g * LANES:(g + 1) * LANES]
        tmp[g, pl.ds(0, n, stride=2), :] = part
        tmp[g, pl.ds(1, n, stride=2), :] = part
    return jnp.concatenate([tmp[g] for g in range(chunks)], axis=1)


def pair_rows(ref, tmp, x0, y0, nx, ny):
    z = ref.shape[2]
    for a in range(nx):
        put_lanes(tmp, a, ref[x0 + 2 * a] + ref[x0 + 2 * a + 1])
    return jnp.concatenate([take_pairs(tmp, a, y0, ny, z // LANES) for a in range(nx)], axis=0)


CORNER_CELLS = ((1, 1), (1, 2), (2, 1))


def put_tiles(out, at, rows):
    n = rows.shape[1] // 8
    for k in range(rows.shape[0]):
        for t in range(n):
            out[(at + k) * n + t] = rows[k, 8 * t:8 * t + 8]


def pack_fine(x_in, b_in, m_in, x, b, m, m3, *outs):
    X, Y = x.shape[0], x.shape[1]
    *outs, tmp, sems = outs
    cx, cy, cz = m3.shape
    copies = []
    for src, dst in ((x_in, x), (b_in, b), (m_in, m)):
        for k in range(PIECES):
            part = pl.ds(k * (X // PIECES), X // PIECES)
            copies.append(pltpu.make_async_copy(src.at[part], dst.at[part], sems.at[len(copies)]))
    for copy in copies:
        copy.start()
    for copy in copies:
        copy.wait()
    gyp, gym, gxp, gxm, cpp, cpm, cmp_, cmm = outs
    for a in range(cx):
        put_lanes(tmp, a, (m[4 * a] + m[4 * a + 1]) + (m[4 * a + 2] + m[4 * a + 3]))
    chunks = tmp.shape[1]
    quads = [jnp.concatenate([(tmp[a, g, pl.ds(0, cy, stride=4), :] + tmp[a, g, pl.ds(1, cy, stride=4), :])
                              + (tmp[a, g, pl.ds(2, cy, stride=4), :] + tmp[a, g, pl.ds(3, cy, stride=4), :])
                              for g in range(chunks)], axis=1) for a in range(cx)]
    coarse = add_pairs(add_pairs(jnp.concatenate(quads, axis=0))) * (1.0 / 64.0)
    m3[...] = coarse.reshape(cx, cy, cz)
    half = cx * cy // 2
    for out in (gyp, gym, gxp, gxm):
        last = out.shape[0] - 1
        out[last, 0:half, 0:cz] = coarse[0:half]
        out[last, 0:half, cz:2 * cz] = coarse[half:2 * half]
    for out in (cpp, cpm, cmp_, cmm):
        for a in range(cx):
            for l in range(cy):
                out[7 + a, :, l * cz:(l + 1) * cz] = coarse[a * cy + l:a * cy + l + 1]
    for out, sl in ((gxp, lambda k: slice(X - k, X)), (gxm, lambda k: slice(0, k))):
        put_tiles(out, 0, x[sl(3)])
        put_tiles(out, 3, b[sl(2)])
        put_tiles(out, 5, m[sl(3)])
    for out, sl in ((gyp, lambda k: slice(Y - k, Y)), (gym, lambda k: slice(0, k))):
        out[0:X, 0:3, :] = x[:, sl(3), :]
        out[0:X, 3:5, :] = b[:, sl(2), :]
        out[0:X, 5:8, :] = m[:, sl(3), :]
    for out, sx, sy in ((cpp, 1, 1), (cpm, 1, -1), (cmp_, -1, 1), (cmm, -1, -1)):
        for k, (di, dj) in enumerate(CORNER_CELLS):
            i = X - di if sx > 0 else di - 1
            j = Y - dj if sy > 0 else dj - 1
            out[k] = x[i, j:j + 1, :]
            out[3 + k] = m[i, j:j + 1, :]
            if k == 0:
                out[6] = b[i, j:j + 1, :]


def smooth_fine(x, b, m, m3, gyl, gyh, gxl, gxh, cll, clh, chl, chh,
                xe, r, kx, ky, kyp, kz, kzp, dg, w, b2, m2, m9, sxp, sxm, syp, sym,
                be, me, u, tmp, tmp2):
    X, Y, Z = x.shape
    R = X + 2 * FX
    x_end, y_end = FX + X, FY + Y
    for ext, own, lo, n in ((xe, x, 0, 3), (be, b, 3, 2), (me, m, 5, 3)):
        kept = halved if ext is me else plain
        ext[FX:x_end, FY:y_end, :] = kept(own[...])
        for msg, r0 in ((gxl, FX - n), (gxh, x_end)):
            for k in range(n):
                for t in range(Y // 8):
                    ext[r0 + k, FY + 8 * t:FY + 8 * t + 8, :] = kept(msg[(lo + k) * (Y // 8) + t])
        ext[FX:x_end, FY - n:FY, :] = kept(gyl[0:X, lo:lo + n, :])
        ext[FX:x_end, y_end:y_end + n, :] = kept(gyh[0:X, lo:lo + n, :])
    for msg, sx, sy in ((cll, -1, -1), (clh, -1, 1), (chl, 1, -1), (chh, 1, 1)):
        for k, (di, dj) in enumerate(CORNER_CELLS):
            i = x_end - 1 + di if sx > 0 else FX - di
            j = y_end - 1 + dj if sy > 0 else FY - dj
            xe[i, j:j + 1, :] = msg[k]
            me[i, j:j + 1, :] = 0.5 * msg[3 + k]
            if k == 0:
                be[i, j:j + 1, :] = msg[6]
    co = (kx, ky, kyp, kz, kzp, dg, w)
    coefficients(me, co, R, SHIFT, UF)

    def first(i, carry):
        ax, _ = apply_row(xe, co, i)
        res = be[i] - ax
        r[i] = res
        u[i] = w[i] * res
        return carry

    loop(1, R - 1, first, 0, UF)

    def second(i, carry):
        au, c = apply_row(u, co, i)
        res = r[i] - au
        r[i] = res
        up = ALPHA * c + BETA * (w[i] * res)
        xe[i] = xe[i] + c + up
        be[i] = up
        return carry

    loop(2, R - 2, second, 0, UF)

    def third(i, carry):
        au, _ = apply_row(be, co, i)
        r[i] = r[i] - au
        return carry

    loop(3, R - 3, third, 0, UF)
    nx, ny, nz = X // 2, Y // 2, Z // 2
    sums = jnp.concatenate([pair_rows(r, tmp, FX, FY, nx, ny), pair_rows(me, tmp2, FX - 2, 0, nx + 2, ny + 4)], axis=0)
    sums = add_pairs(sums)
    b2[...] = 0.5 * sums[0:nx * ny].reshape(nx, ny, nz)
    mm = 0.25 * sums[nx * ny:].reshape(nx + 2, ny + 4, nz)
    cells = mm[1:nx + 1, 2:2 + ny, :]
    m2[...] = cells
    fz = 0.5 * (cells + nxt(cells, 2))
    fzp = prv(fz, 2)
    diag = (4.0 * SHIFT + 0.5 * (4.0 * cells + mm[0:nx, 2:2 + ny, :] + mm[2:nx + 2, 2:2 + ny, :]
                                 + mm[1:nx + 1, 1:1 + ny, :] + mm[1:nx + 1, 3:3 + ny, :]) + (fz + fzp))
    u2 = (b2[...] * (1.0 / diag)) * INV_C
    bb = b2[...]
    sxp[0:1] = u2[nx - 4:nx - 3]
    sxp[1:4] = bb[nx - 3:nx]
    sxp[4:8] = cells[nx - 4:nx]
    sxm[0:3] = bb[0:3]
    sxm[3:4] = u2[3:4]
    sxm[4:8] = cells[0:4]
    syp[0:nx, 0:1, :] = u2[:, ny - 4:ny - 3, :]
    syp[0:nx, 1:4, :] = bb[:, ny - 3:ny, :]
    syp[0:nx, 4:8, :] = cells[:, ny - 4:ny, :]
    sym[0:nx, 0:3, :] = bb[:, 0:3, :]
    sym[0:nx, 3:4, :] = u2[:, 3:4, :]
    sym[0:nx, 4:8, :] = cells[:, 0:4, :]
    for dst, src in ((sxp, r[FX + X - 1, FY:y_end]), (sxm, r[FX, FY:y_end])):
        for h in range(2):
            for g in range(2):
                dst[8 + 2 * h + g] = src[h * ny:(h + 1) * ny, g * nz:(g + 1) * nz]
    for dst, j in ((syp, Y - 1), (sym, 0)):
        for h in range(2):
            for k in range(ny):
                row = r[FX + h * ny + k, FY + j:FY + j + 1, :]
                for g in range(2):
                    dst[nx + 2 * h + g, k:k + 1, :] = row[:, g * nz:(g + 1) * nz]
    for out, j0, step in ((syp, ny - 1, -1), (sym, 0, 1)):
        for t in range(3):
            j = j0 + step * t
            out[nx + 4, t:t + 1, :] = u2[nx - 4 + t, j:j + 1, :]
            out[nx + 4, 3 + t:4 + t, :] = u2[3 - t, j:j + 1, :]
    cx, cy, cz = m3.shape
    half = cx * cy // 2
    m9[:, 3 * cy:4 * cy, :] = jnp.ones((3 * cx, cy, cz), F32)
    m9[cx:2 * cx, cy:2 * cy, :] = m3[...]
    for msg, c0 in ((gyl, 0), (gyh, 2 * cy)):
        both = jnp.concatenate([msg[X, 0:half, 0:cz], msg[X, 0:half, cz:2 * cz]], axis=0)
        m9[cx:2 * cx, c0:c0 + cy, :] = both.reshape(cx, cy, cz)
    for msg, r0 in ((gxl, 0), (gxh, 2 * cx)):
        both = jnp.concatenate([msg[Y, 0:half, 0:cz], msg[Y, 0:half, cz:2 * cz]], axis=0)
        m9[r0:r0 + cx, cy:2 * cy, :] = both.reshape(cx, cy, cz)
    for msg, r0, c0 in ((cll, 0, 0), (clh, 0, 2 * cy), (chl, 2 * cx, 0), (chh, 2 * cx, 2 * cy)):
        for a in range(cx):
            for l in range(cy):
                m9[r0 + a, c0 + l:c0 + l + 1, :] = msg[7 + a, :, l * cz:(l + 1) * cz]
    for out, line in ((syp, cy - 1), (sym, 2 * cy)):
        for k in range(3 * cx):
            out[nx + 5, k % ny:k % ny + 1, (k // ny) * cz:(k // ny + 1) * cz] = m9[k, line:line + 1, :]


def far_lines(row, k, gyl, gyh):
    cz, ny = row.shape[1], gyl.shape[1]
    nx = gyl.shape[0] - 6
    col = lax.broadcasted_iota(jnp.int32, row.shape, 0)
    pick = lambda msg: msg[nx + 5, k % ny:k % ny + 1, (k // ny) * cz:(k // ny + 1) * cz]
    row = jnp.where(col == 3 * row.shape[0] // 4, pick(gyh), row)
    return jnp.where(col == row.shape[0] - 1, pick(gyl), row)


def spread_rows(gyl, gyh, sxp, sxm, m9, axp, axm):
    ny, nx = sxp.shape[1], gyl.shape[0] - 6
    cx, cz = m9.shape[0] // 3, m9.shape[2]
    for out, k in ((axp, cx - 1), (axm, 2 * cx)):
        out[10, :, 0:cz] = far_lines(m9[k], k, gyl, gyh)
    yend = MX + ny
    for own, out, r0, line in ((sxp, axp, nx - 4, 0), (sxm, axm, 0, 3)):
        for lo in (0, 4):
            out[lo:lo + 4, MX:yend, :] = own[lo:lo + 4]
            out[lo:lo + 4, 0:MX, :] = gyl[r0:r0 + 4, lo:lo + 4, :]
            out[lo:lo + 4, yend:yend + MX, :] = gyh[r0:r0 + 4, lo:lo + 4, :]
        for t in range(3):
            row = t if line == 0 else 3 - t
            out[row, 3 - t:4 - t, :] = gyl[nx + 4, line + t:line + t + 1, :]
            out[row, yend + t:yend + t + 1, :] = gyh[nx + 4, line + t:line + t + 1, :]
        for h in range(2):
            for g in range(2):
                out[8 + g, h * ny:(h + 1) * ny, :] = own[8 + 2 * h + g]


def smooth_mid(b2, m2, m3, test, w3, gxl, gxh, gyl, gyh,
               xm, rm, kx, ky, kyp, kz, kzp, dg, w, out,
               qe, me, u, tmp):
    nx, ny, nz = b2.shape
    R = nx + 2 * MX
    shift = 4.0 * SHIFT
    xend, yend = MX + nx, MX + ny
    for ext, own, lo in ((qe, b2, 0), (me, m2, 4)):
        kept = halved if ext is me else plain
        ext[MX:xend, MX:yend, :] = kept(own[...])
        ext[MX:xend, 0:MX, :] = kept(gyl[0:nx, lo:lo + 4, :])
        ext[MX:xend, yend:yend + MX, :] = kept(gyh[0:nx, lo:lo + 4, :])
        ext[0:MX] = kept(gxl[lo:lo + 4])
        ext[xend:xend + MX] = kept(gxh[lo:lo + 4])
    co = (kx, ky, kyp, kz, kzp, dg, w)
    coefficients(me, co, R, shift, UM)
    col = lax.broadcasted_iota(jnp.int32, (ny + 2 * MX, nz), 0)
    dcol = jnp.maximum(jnp.maximum(MX - col, col - (yend - 1)), 0)

    def first(i, carry):
        di = jnp.maximum(jnp.maximum(MX - i, i - (xend - 1)), 0)
        q = qe[i]
        sent = (dcol + di == 5) | (dcol == 4) | (di == 4)
        u[i] = jnp.where(sent, q, w[i] * q)
        return carry

    u[0] = qe[0]
    u[R - 1] = qe[R - 1]
    loop(1, R - 1, first, 0, UM)

    def second(i, carry):
        au, c = apply_row(u, co, i)
        res = qe[i] - au
        rm[i] = res
        up = ALPHA * c + BETA * (w[i] * res)
        xm[i] = c + up
        qe[i] = up
        return carry

    loop(1, R - 1, second, 0, UM)

    def third(i, carry):
        au, _ = apply_row(qe, co, i)
        rm[i] = rm[i] - au
        return carry

    loop(2, R - 2, third, 0, UM)
    cx, cy = nx // 2, ny // 2
    b3 = 0.5 * add_pairs(pair_rows(rm, tmp, MX, MX, cx, cy)).reshape(cx, cy, nz // 2)
    cz = nz // 2
    kept = jnp.sum(jnp.sum(test[...] * b3, axis=0), axis=0, keepdims=True)
    mass = jnp.sum(jnp.sum(m3[...], axis=0), axis=0, keepdims=True)
    lane = lax.broadcasted_iota(jnp.int32, (1, cz), 1)
    extra = jnp.where(lane < cz // 2, kept + pltpu.roll(kept, cz // 2, 1), mass + pltpu.roll(mass, cz // 2, 1))
    lines = jnp.concatenate([(w3[...] * b3).reshape(cx * cy, cz), extra], axis=0)
    both = lines.reshape(cx * cy + 1, 1, cz)

    def put(k, carry):
        out[k] = both
        return carry

    lax.fori_loop(0, out.shape[0], put, 0)


def plane(f, zs):
    c1 = zs + (nxt(f, 0) + prv(f, 0))
    c2 = nxt(zs, 0) + prv(zs, 0)
    return 0.5 * c1 + 0.125 * c2, 0.5 * f + 0.125 * c1 + 0.0625 * c2


def weighted_sums(f, m, mzn, mzp, lo, hi):
    own, out = {}, {}
    for i in range(lo - 1, hi + 1):
        fn, fp = nxt(f[i], 1), prv(f[i], 1)
        a, o = plane(f[i], fn + fp)
        am, om = plane(m[i] * f[i], mzn[i] * fn + mzp[i] * fp)
        own[i], out[i] = (a, am), (o, om)
    return {i: m[i] * (own[i][0] + (out[i - 1][0] + out[i + 1][0])) + (own[i][1] + (out[i - 1][1] + out[i + 1][1]))
            for i in range(lo, hi)}


def rotate_rows(m, rows, mzn, mzp):
    for i in range(rows):
        mzn[i] = nxt(m[i], 1)
        mzp[i] = prv(m[i], 1)


def inverse_rows(m, mzn, mzp, lo, hi):
    planes = {i: plane(m[i], mzn[i] + mzp[i]) for i in range(lo - 1, hi + 1)}
    return {i: JACOBI / (16.0 * SHIFT + 0.5 * (WEIGHT_TOTAL * m[i] + (planes[i][0] + (planes[i - 1][1] + planes[i + 1][1]))))
            for i in range(lo, hi)}


def mean_weights(m9, test, w3, mzn, mzp):
    rows, (cx, cy, cz) = m9.shape[0], test.shape
    rotate_rows(m9, rows, mzn, mzp)
    w = inverse_rows(m9, mzn, mzp, 1, rows - 1)
    one = jnp.ones(m9.shape[1:], F32)
    g = {i: one for i in range(1, rows - 1)}
    total = {i: one for i in range(cx, 2 * cx)}
    for sweep in range(SWEEPS - 1):
        lo, hi = 2 + sweep, rows - 2 - sweep
        sums = weighted_sums({i: w[i] * g[i] for i in range(lo - 1, hi + 1)}, m9, mzn, mzp, lo, hi)
        g = {i: (1.0 - JACOBI) * g[i] + 0.5 * sums[i] for i in range(lo, hi)}
        total = {i: total[i] + g[i] for i in total}
    for i in range(cx):
        wi = w[cx + i]
        test[i] = (1.0 - 16.0 * SHIFT * (wi * total[cx + i]))[cy:2 * cy]
        w3[i] = wi[cy:2 * cy]


def coarse_weights(m9, gyl, gyh, gxl, gxh, mw, mzn, mzp, wc):
    rows, cz = mw.shape[0], mw.shape[2]
    mw[0] = gxl[10, :, 0:cz]
    mw[rows - 1] = gxh[10, :, 0:cz]
    for k in range(rows - 2):
        mw[1 + k] = far_lines(m9[k], k, gyl, gyh)
    rotate_rows(mw, rows, mzn, mzp)
    w = inverse_rows(mw, mzn, mzp, 1, rows - 1)
    for i in w:
        wc[i] = w[i]


def finish(got, m9, xm, rm, kx2, ky2, kyp2, kz2, kzp2, dg2, w2, x1, r1, gxl, gxh, gyl, gyh,
           kx, ky, kyp, kz, kzp, dg, w, new,
           ec, mw, mzn, mzp, wc, vm, um, t2, t3, vf, uf, qf, of, sems):
    X, Y, Z = of.shape
    nx, ny, nz = X // 2, Y // 2, Z // 2
    cx, cy, cz = nx // 2, ny // 2, nz // 2
    NX, NY = lax.axis_size("gx"), lax.axis_size("gy")
    px, py = lax.axis_index("gx"), lax.axis_index("gy")
    CY = ec.shape[1]
    rows = 3 * cx + 2
    coarse_weights(m9, gyl, gyh, gxl, gxh, mw, mzn, mzp, wc)

    for k in range(-2, 3):
        gx = lax.rem(px + k + NX, NX) * NY
        take = slice(cx - 1, cx) if k == -2 else slice(0, 1) if k == 2 else slice(0, cx)
        r0 = (k + 1) * cx + 1 if k > -2 else 0
        n = take.stop - take.start
        for l in range(-2, 3):
            slot = gx + lax.rem(py + l + NY, NY)
            for a in range(n):
                lines = got[slot, pl.ds((take.start + a) * cy, cy), 0, :]
                if l == -2:
                    ec[r0 + a, CY - 1:CY, :] = lines[cy - 1:cy]
                elif l == 2:
                    ec[r0 + a, 3 * cy:CY - 1, :] = lines[0:cy - 1]
                else:
                    ec[r0 + a, (l + 1) * cy:(l + 2) * cy, :] = lines
    e = {i: ec[i] for i in range(rows)}
    for sweep in range(SWEEPS - 1):
        lo, hi = 1 + sweep, rows - 1 - sweep
        sums = weighted_sums(e, mw, mzn, mzp, lo, hi)
        e = {i: (1.0 - JACOBI) * e[i] + (ec[i] + (0.5 * wc[i]) * sums[i]) for i in range(lo, hi)}
    sums = got[0, cx * cy]
    for k in range(1, NX * NY):
        sums = sums + got[k, cx * cy]
    cells = cx * cy * cz * NX * NY
    first = lax.broadcasted_iota(jnp.int32, (1, cz), 1) < cz // 2
    total = jnp.sum(jnp.where(first, sums, 0.0), axis=1, keepdims=True) * (1.0 / cells)
    mean_m = jnp.sum(jnp.where(first, 0.0, sums), axis=1, keepdims=True) * (1.0 / cells)
    kappa = JACOBI * total / (16.0 * SHIFT + WEIGHT_TOTAL * mean_m)

    ex, ey = cx + 4, cy + 4
    e = jnp.concatenate([e[cx - 1 + i] + kappa for i in range(ex)], axis=0)
    ed = double(e).reshape(ex, CY, nz)[:, cy - 2:cy - 2 + ey, :]
    for a in range(ex):
        both = repeat_rows(t2, ed[a])
        vm[2 * a] = both
        vm[2 * a + 1] = both
    R = nx + 2 * MX
    co2 = (kx2, ky2, kyp2, kz2, kzp2, dg2, w2)
    co = (kx, ky, kyp, kz, kzp, dg, w)

    def mid_first(i, carry):
        au, c = apply_row(vm, co2, i)
        res = rm[i] - au
        upd = w2[i] * res
        rm[i] = res
        um[i] = upd
        xm[i] = xm[i] + c + upd
        return carry

    loop(2, R - 2, mid_first, 0, UM)

    def mid_second(i, carry):
        au, c = apply_row(um, co2, i)
        xm[i] = xm[i] + (ALPHA * c + BETA * (w2[i] * (rm[i] - au)))
        return carry

    loop(3, R - 3, mid_second, 0, UM)

    ye = Y + 2 * FY
    wide = nx + 2
    big = double(xm[MX - 1:MX - 1 + wide].reshape(wide * (ny + 2 * MX), nz))
    big = big.reshape(wide, ny + 2 * MX, Z)[:, MX - 2:MX - 2 + ny + 4, :]
    for a in range(wide):
        both = repeat_rows(t3, big[a])
        vf[1 + 2 * a] = both
        vf[2 + 2 * a] = both
    RF = X + 2 * FX
    uf[...] = r1[...]
    for row, msg in ((FX - 1, gxl), (FX + X, gxh)):
        for g in range(2):
            uf[row, FY:FY + Y, g * nz:(g + 1) * nz] = msg[8 + g]
    for colj, msg in ((FY - 1, gyl), (FY + Y, gyh)):
        for h in range(2):
            for k in range(ny):
                for g in range(2):
                    uf[FX + h * ny + k, colj:colj + 1, g * nz:(g + 1) * nz] = msg[nx + 2 * h + g, k:k + 1, :]

    def fine_first(i, carry):
        au, _ = apply_row(vf, co, i)
        res = uf[i] - au
        uf[i] = res
        qf[i] = w[i] * res
        return carry

    loop(2, RF - 2, fine_first, 0, UF)

    def fine_second(i, carry):
        au, c = apply_row(qf, co, i)
        upd = vf[i] + ((1.0 + ALPHA) * c + BETA * (w[i] * (uf[i] - au)))
        of[i - FX] = (x1[i] + upd)[FY:FY + Y]
        return carry

    part = X // PIECES
    copies = []
    for k in range(PIECES):
        lo = k * part
        loop(FX + lo, FX + lo + part, fine_second, 0, UF)
        src = of.at[pl.ds(lo, part)]
        copies.append(pltpu.make_async_copy(src, new.at[pl.ds(lo, part)], sems.at[k]))
        copies[-1].start()
    for copy in copies:
        copy.wait()


def vmem_call(body, name, out_shape, scratch, inputs, hbm_in=0, hbm_out=False):
    space = pl.BlockSpec(memory_space=pltpu.VMEM)
    far = pl.BlockSpec(memory_space=pltpu.HBM)
    single = not isinstance(out_shape, (list, tuple))
    return pl.pallas_call(
        body,
        name=name,
        out_shape=out_shape,
        in_specs=[far] * hbm_in + [space] * (len(inputs) - hbm_in),
        out_specs=(far if hbm_out else space) if single else [space] * len(out_shape),
        scratch_shapes=scratch,
        compiler_params=pltpu.CompilerParams(vmem_limit_bytes=VMEM_LIMIT),
    )(*inputs)


X_DIRS = ((1, 0), (-1, 0))
Y_DIRS = ((0, 1), (0, -1))
CORNERS = ((1, 1), (1, -1), (-1, 1), (-1, -1))


def exchange(messages, dirs):
    nx, ny = lax.axis_size("gx"), lax.axis_size("gy")
    got = []
    for msg, (dx, dy) in zip(messages, dirs):
        pairs = [(i * ny + j, ((i + dx) % nx) * ny + (j + dy) % ny) for i in range(nx) for j in range(ny)]
        got.append(lax.ppermute(msg, ("gx", "gy"), pairs))
    return got


def sd(*shape):
    return jax.ShapeDtypeStruct(shape, F32)


def vm(*shape):
    return pltpu.VMEM(shape, F32)


def local(pressure, divergence, inverse_density):
    X, Y, Z = pressure.shape
    nx, ny, nz = X // 2, Y // 2, Z // 2
    cx, cy, cz = nx // 2, ny // 2, nz // 2
    NX, NY = lax.axis_size("gx"), lax.axis_size("gy")
    xe, ye = X + 2 * FX, Y + 2 * FY
    mxe, mye = nx + 2 * MX, ny + 2 * MX
    fine = tuple(pltpu.with_memory_space_constraint(a, pltpu.HBM) for a in (pressure, divergence, inverse_density))
    msgs = vmem_call(pack_fine, "pack_fine",
                     [sd(X, Y, Z)] * 3 + [sd(cx, cy, cz)] + [sd(X + 1, 8, Z)] * 2 + [sd(Y + 1, 8, Z)] * 2 + [sd(7 + cx, 1, Z)] * 4,
                     [vm(cx, Z // LANES, Y, LANES), pltpu.SemaphoreType.DMA((3 * PIECES,))], fine, hbm_in=3)
    got = exchange(msgs[4:], Y_DIRS + X_DIRS + CORNERS)
    res = vmem_call(
        smooth_fine, "smooth_fine",
        [sd(xe, ye, Z)] * 9 + [sd(nx, ny, nz)] * 2
        + [sd(3 * cx, 4 * cy, cz)] + [sd(12, ny, nz)] * 2 + [sd(nx + 6, 8, nz)] * 2,
        [vm(xe, ye, Z)] * 3 + [vm(nx, Z // LANES, ye, LANES), vm(nx + 2, Z // LANES, ye, LANES)],
        tuple(msgs[:4]) + tuple(got))
    x1, r1 = res[:2]
    fine_co = tuple(res[2:9])
    b2, m2, m9 = res[9:12]
    m3 = msgs[3]
    test, w3 = vmem_call(mean_weights, "mean_weights", [sd(cx, cy, cz)] * 2, [vm(3 * cx, 4 * cy, cz)] * 2, (m9,))
    cols = exchange(res[14:16], Y_DIRS)
    rows = exchange(vmem_call(spread_rows, "spread_rows", [sd(11, mye, nz)] * 2, [],
                              (*cols, *res[12:14], m9)), X_DIRS)
    got2 = rows + cols
    *mid, out = vmem_call(
        smooth_mid, "smooth_mid",
        [sd(mxe, mye, nz)] * 9 + [sd(NX * NY, cx * cy + 1, 1, cz)],
        [vm(mxe, mye, nz)] * 3 + [vm(cx, nz // LANES, mye, LANES)],
        (b2, m2, m3, test, w3) + tuple(got2))
    gathered = lax.all_to_all(out, ("gx", "gy"), 0, 0)
    window = (3 * cx + 2, 4 * cy, cz)
    return vmem_call(
        finish, "finish", sd(X, Y, Z),
        [vm(*window)] * 5 + [vm(mxe, mye, nz)] * 2 + [vm(nz // LANES, mye, LANES), vm(Z // LANES, ye, LANES)]
        + [vm(xe, ye, Z)] * 3 + [vm(X, Y, Z), pltpu.SemaphoreType.DMA((PIECES,))],
        (gathered, m9, *mid, x1, r1) + tuple(got2) + fine_co, hbm_out=True)


def solution(mesh):
    return jax.shard_map(
        local,
        mesh=mesh,
        in_specs=(P("gx", "gy", None),) * 3,
        out_specs=P("gx", "gy", None),
        check_vma=False,
    )
```

```python
import jax
import jax.numpy as jnp
from jax import lax
from jax.experimental import pallas as pl
from jax.experimental.pallas import tpu as pltpu
from jax.sharding import PartitionSpec as P


SWEEPS = 4
SHIFT = 0.05
CENTER = (2.0 + 0.3) / 2
HALF = (2.0 - 0.3) / 2
Q0 = CENTER / HALF
P0 = 1.0 / Q0
P1 = 1.0 / (2.0 * Q0 - P0)
ALPHA = P1 * P0
BETA = 2.0 * P1 / HALF * CENTER
INV_C = 1.0 / CENTER
JACOBI = 0.8
WEIGHT_TOTAL = 5.0

FX = 3
FY = 4
MX = 4

F32 = jnp.float32
UF = 20
UM = 14
PIECES = 4
VMEM_LIMIT = 20 * 1024 * 1024


def nxt(v, axis):
    return pltpu.roll(v, v.shape[axis] - 1, axis)


def prv(v, axis):
    return pltpu.roll(v, 1, axis)


def loop(low, high, body, init, unroll):
    rest = (high - low) % unroll
    carry = init
    for k in range(rest):
        carry = body(low + k, carry)
    start = low + rest

    def group(g, c):
        for k in range(unroll):
            c = body(start + g * unroll + k, c)
        return c

    return lax.fori_loop(0, (high - start) // unroll, group, carry)


def plain(a):
    return a


def halved(a):
    return 0.5 * a


def coefficients(m_ref, k, rows, shift, unroll):
    kx, ky, kyp, kz, kzp, d_ref, w_ref = k
    kx[0] = m_ref[0] + m_ref[1]

    def body(i, carry):
        m = m_ref[i]
        fx = m + m_ref[i + 1]
        fxp = m + m_ref[i - 1]
        fz = m + nxt(m, 1)
        fzp = m + prv(m, 1)
        fy = m + nxt(m, 0)
        fyp = m + prv(m, 0)
        kx[i] = fx
        ky[i] = fy
        kyp[i] = fyp
        kz[i] = fz
        kzp[i] = fzp
        d = shift + ((fx + fxp) + (fy + fyp) + (fz + fzp))
        d_ref[i] = d
        w_ref[i] = INV_C / d
        return carry

    loop(1, rows - 1, body, 0, unroll)


def apply_row(v_ref, k, i):
    kx, ky, kyp, kz, kzp, d_ref, _ = k
    c = v_ref[i]
    z = kz[i] * nxt(c, 1) + kzp[i] * prv(c, 1)
    y = ky[i] * nxt(c, 0) + kyp[i] * prv(c, 0)
    x = kx[i] * v_ref[i + 1] + kx[i - 1] * v_ref[i - 1]
    return d_ref[i] * c - ((x + y) + z), c


BF16 = jnp.bfloat16


def select(a, table):
    hi = a.astype(BF16)
    rest = a - hi.astype(F32)
    mid = rest.astype(BF16)
    low = (rest - mid.astype(F32)).astype(BF16)
    n = a.shape[0]
    out = jnp.dot(jnp.concatenate([hi, mid, low], axis=0), table, preferred_element_type=F32)
    return (out[0:n] + out[n:2 * n]) + out[2 * n:3 * n]


def chunks_as_rows(a, width):
    return jnp.concatenate([a[:, g * width:(g + 1) * width] for g in range(a.shape[1] // width)], axis=0)


def rows_as_chunks(a, count):
    n = a.shape[0] // count
    return jnp.concatenate([a[g * n:(g + 1) * n] for g in range(count)], axis=1)


def add_pairs(a):
    row = lax.broadcasted_iota(jnp.int32, (2 * LANES, LANES), 0)
    col = lax.broadcasted_iota(jnp.int32, (2 * LANES, LANES), 1)
    table = jnp.where(row // 2 == col, 1.0, 0.0).astype(BF16)
    return rows_as_chunks(select(chunks_as_rows(a, 2 * LANES), table), a.shape[1] // (2 * LANES))


def double(a):
    row = lax.broadcasted_iota(jnp.int32, (LANES, 2 * LANES), 0)
    col = lax.broadcasted_iota(jnp.int32, (LANES, 2 * LANES), 1)
    table = jnp.where(col // 2 == row, 1.0, 0.0).astype(BF16)
    return rows_as_chunks(select(chunks_as_rows(a, LANES), table), a.shape[1] // LANES)


LANES = 128


def put_lanes(tmp, a, val):
    for g in range(val.shape[1] // LANES):
        tmp[a, g] = val[:, g * LANES:(g + 1) * LANES]


def take_pairs(tmp, a, y0, ny, chunks):
    parts = [tmp[a, g, pl.ds(y0, ny, stride=2), :] + tmp[a, g, pl.ds(y0 + 1, ny, stride=2), :] for g in range(chunks)]
    return jnp.concatenate(parts, axis=1)


def repeat_rows(tmp, val):
    n, chunks = val.shape[0], val.shape[1] // LANES
    for g in range(chunks):
        part = val[:, g * LANES:(g + 1) * LANES]
        tmp[g, pl.ds(0, n, stride=2), :] = part
        tmp[g, pl.ds(1, n, stride=2), :] = part
    return jnp.concatenate([tmp[g] for g in range(chunks)], axis=1)


def pair_rows(ref, tmp, x0, y0, nx, ny):
    z = ref.shape[2]
    for a in range(nx):
        put_lanes(tmp, a, ref[x0 + 2 * a] + ref[x0 + 2 * a + 1])
    return jnp.concatenate([take_pairs(tmp, a, y0, ny, z // LANES) for a in range(nx)], axis=0)


CORNER_CELLS = ((1, 1), (1, 2), (2, 1))


def put_tiles(out, at, rows):
    n = rows.shape[1] // 8
    for k in range(rows.shape[0]):
        for t in range(n):
            out[(at + k) * n + t] = rows[k, 8 * t:8 * t + 8]


def pack_fine(x_in, b_in, m_in, x, b, m, m3, *outs):
    X, Y = x.shape[0], x.shape[1]
    *outs, tmp, sems = outs
    cx, cy, cz = m3.shape
    copies = []
    for src, dst in ((m_in, m), (x_in, x), (b_in, b)):
        for k in range(PIECES):
            part = pl.ds(k * (X // PIECES), X // PIECES)
            copies.append(pltpu.make_async_copy(src.at[part], dst.at[part], sems.at[len(copies)]))
    for copy in copies:
        copy.start()
    for copy in copies[:PIECES]:
        copy.wait()
    gyp, gym, gxp, gxm, cpp, cpm, cmp_, cmm = outs
    for a in range(cx):
        put_lanes(tmp, a, (m[4 * a] + m[4 * a + 1]) + (m[4 * a + 2] + m[4 * a + 3]))
    chunks = tmp.shape[1]
    quads = [jnp.concatenate([(tmp[a, g, pl.ds(0, cy, stride=4), :] + tmp[a, g, pl.ds(1, cy, stride=4), :])
                              + (tmp[a, g, pl.ds(2, cy, stride=4), :] + tmp[a, g, pl.ds(3, cy, stride=4), :])
                              for g in range(chunks)], axis=1) for a in range(cx)]
    coarse = add_pairs(add_pairs(jnp.concatenate(quads, axis=0))) * (1.0 / 64.0)
    m3[...] = coarse.reshape(cx, cy, cz)
    half = cx * cy // 2
    for out in (gyp, gym, gxp, gxm):
        last = out.shape[0] - 1
        out[last, 0:half, 0:cz] = coarse[0:half]
        out[last, 0:half, cz:2 * cz] = coarse[half:2 * half]
    for out in (cpp, cpm, cmp_, cmm):
        for a in range(cx):
            for l in range(cy):
                out[7 + a, :, l * cz:(l + 1) * cz] = coarse[a * cy + l:a * cy + l + 1]
    for copy in copies[PIECES:]:
        copy.wait()
    for out, sl in ((gxp, lambda k: slice(X - k, X)), (gxm, lambda k: slice(0, k))):
        put_tiles(out, 0, x[sl(3)])
        put_tiles(out, 3, b[sl(2)])
        put_tiles(out, 5, m[sl(3)])
    for out, sl in ((gyp, lambda k: slice(Y - k, Y)), (gym, lambda k: slice(0, k))):
        out[0:X, 0:3, :] = x[:, sl(3), :]
        out[0:X, 3:5, :] = b[:, sl(2), :]
        out[0:X, 5:8, :] = m[:, sl(3), :]
    for out, sx, sy in ((cpp, 1, 1), (cpm, 1, -1), (cmp_, -1, 1), (cmm, -1, -1)):
        for k, (di, dj) in enumerate(CORNER_CELLS):
            i = X - di if sx > 0 else di - 1
            j = Y - dj if sy > 0 else dj - 1
            out[k] = x[i, j:j + 1, :]
            out[3 + k] = m[i, j:j + 1, :]
            if k == 0:
                out[6] = b[i, j:j + 1, :]


def smooth_fine(x, b, m, m3, gyl, gyh, gxl, gxh, cll, clh, chl, chh,
                xe, r, kx, ky, kyp, kz, kzp, dg, w, b2, m2, m9, sxp, sxm, syp, sym, ryp, rym,
                be, me, u, tmp, tmp2):
    X, Y, Z = x.shape
    R = X + 2 * FX
    x_end, y_end = FX + X, FY + Y
    for ext, own, lo, n in ((xe, x, 0, 3), (be, b, 3, 2), (me, m, 5, 3)):
        kept = halved if ext is me else plain
        ext[FX:x_end, FY:y_end, :] = kept(own[...])
        for msg, r0 in ((gxl, FX - n), (gxh, x_end)):
            for k in range(n):
                for t in range(Y // 8):
                    ext[r0 + k, FY + 8 * t:FY + 8 * t + 8, :] = kept(msg[(lo + k) * (Y // 8) + t])
        ext[FX:x_end, FY - n:FY, :] = kept(gyl[0:X, lo:lo + n, :])
        ext[FX:x_end, y_end:y_end + n, :] = kept(gyh[0:X, lo:lo + n, :])
    for msg, sx, sy in ((cll, -1, -1), (clh, -1, 1), (chl, 1, -1), (chh, 1, 1)):
        for k, (di, dj) in enumerate(CORNER_CELLS):
            i = x_end - 1 + di if sx > 0 else FX - di
            j = y_end - 1 + dj if sy > 0 else FY - dj
            xe[i, j:j + 1, :] = msg[k]
            me[i, j:j + 1, :] = 0.5 * msg[3 + k]
            if k == 0:
                be[i, j:j + 1, :] = msg[6]
    co = (kx, ky, kyp, kz, kzp, dg, w)
    coefficients(me, co, R, SHIFT, UF)

    def first(i, carry):
        ax, _ = apply_row(xe, co, i)
        res = be[i] - ax
        r[i] = res
        u[i] = w[i] * res
        return carry

    loop(1, R - 1, first, 0, UF)

    def second(i, carry):
        au, c = apply_row(u, co, i)
        res = r[i] - au
        r[i] = res
        up = ALPHA * c + BETA * (w[i] * res)
        xe[i] = xe[i] + c + up
        be[i] = up
        return carry

    loop(2, R - 2, second, 0, UF)

    def third(i, carry):
        au, _ = apply_row(be, co, i)
        r[i] = r[i] - au
        return carry

    loop(3, R - 3, third, 0, UF)
    nx, ny, nz = X // 2, Y // 2, Z // 2
    sums = jnp.concatenate([pair_rows(r, tmp, FX, FY, nx, ny), pair_rows(me, tmp2, FX - 2, 0, nx + 2, ny + 4)], axis=0)
    sums = add_pairs(sums)
    b2[...] = 0.5 * sums[0:nx * ny].reshape(nx, ny, nz)
    mm = 0.25 * sums[nx * ny:].reshape(nx + 2, ny + 4, nz)
    cells = mm[1:nx + 1, 2:2 + ny, :]
    m2[...] = cells
    fz = 0.5 * (cells + nxt(cells, 2))
    fzp = prv(fz, 2)
    diag = (4.0 * SHIFT + 0.5 * (4.0 * cells + mm[0:nx, 2:2 + ny, :] + mm[2:nx + 2, 2:2 + ny, :]
                                 + mm[1:nx + 1, 1:1 + ny, :] + mm[1:nx + 1, 3:3 + ny, :]) + (fz + fzp))
    u2 = (b2[...] * (1.0 / diag)) * INV_C
    bb = b2[...]
    sxp[0:1] = u2[nx - 4:nx - 3]
    sxp[1:4] = bb[nx - 3:nx]
    sxp[4:8] = cells[nx - 4:nx]
    sxm[0:3] = bb[0:3]
    sxm[3:4] = u2[3:4]
    sxm[4:8] = cells[0:4]
    syp[0:nx, 0:1, :] = u2[:, ny - 4:ny - 3, :]
    syp[0:nx, 1:4, :] = bb[:, ny - 3:ny, :]
    syp[0:nx, 4:8, :] = cells[:, ny - 4:ny, :]
    sym[0:nx, 0:3, :] = bb[:, 0:3, :]
    sym[0:nx, 3:4, :] = u2[:, 3:4, :]
    sym[0:nx, 4:8, :] = cells[:, 0:4, :]
    for dst, src in ((sxp, r[FX + X - 1, FY:y_end]), (sxm, r[FX, FY:y_end])):
        for h in range(2):
            for g in range(2):
                dst[8 + 2 * h + g] = src[h * ny:(h + 1) * ny, g * nz:(g + 1) * nz]
    for dst, j in ((ryp, Y - 1), (rym, 0)):
        for i in range(X):
            dst[i // 8, i % 8:i % 8 + 1, :] = r[FX + i, FY + j:FY + j + 1, :]
    for out, j0, step in ((syp, ny - 1, -1), (sym, 0, 1)):
        for t in range(3):
            j = j0 + step * t
            out[nx, t:t + 1, :] = u2[nx - 4 + t, j:j + 1, :]
            out[nx, 3 + t:4 + t, :] = u2[3 - t, j:j + 1, :]
    cx, cy, cz = m3.shape
    half = cx * cy // 2
    m9[:, 3 * cy:4 * cy, :] = jnp.ones((3 * cx, cy, cz), F32)
    m9[cx:2 * cx, cy:2 * cy, :] = m3[...]
    for msg, c0 in ((gyl, 0), (gyh, 2 * cy)):
        both = jnp.concatenate([msg[X, 0:half, 0:cz], msg[X, 0:half, cz:2 * cz]], axis=0)
        m9[cx:2 * cx, c0:c0 + cy, :] = both.reshape(cx, cy, cz)
    for msg, r0 in ((gxl, 0), (gxh, 2 * cx)):
        both = jnp.concatenate([msg[Y, 0:half, 0:cz], msg[Y, 0:half, cz:2 * cz]], axis=0)
        m9[r0:r0 + cx, cy:2 * cy, :] = both.reshape(cx, cy, cz)
    for msg, r0, c0 in ((cll, 0, 0), (clh, 0, 2 * cy), (chl, 2 * cx, 0), (chh, 2 * cx, 2 * cy)):
        for a in range(cx):
            for l in range(cy):
                m9[r0 + a, c0 + l:c0 + l + 1, :] = msg[7 + a, :, l * cz:(l + 1) * cz]
    for out, line in ((syp, cy - 1), (sym, 2 * cy)):
        for k in range(3 * cx):
            out[nx + 1, k % ny:k % ny + 1, (k // ny) * cz:(k // ny + 1) * cz] = m9[k, line:line + 1, :]


def far_lines(row, k, gyl, gyh):
    cz, ny = row.shape[1], gyl.shape[1]
    nx = gyl.shape[0] - 2
    col = lax.broadcasted_iota(jnp.int32, row.shape, 0)
    pick = lambda msg: msg[nx + 1, k % ny:k % ny + 1, (k // ny) * cz:(k // ny + 1) * cz]
    row = jnp.where(col == 3 * row.shape[0] // 4, pick(gyh), row)
    return jnp.where(col == row.shape[0] - 1, pick(gyl), row)


def spread_rows(gyl, gyh, sxp, sxm, m9, axp, axm):
    ny, nx = sxp.shape[1], gyl.shape[0] - 2
    cx, cz = m9.shape[0] // 3, m9.shape[2]
    for out, k in ((axp, cx - 1), (axm, 2 * cx)):
        out[10, :, 0:cz] = far_lines(m9[k], k, gyl, gyh)
    yend = MX + ny
    for own, out, r0, line in ((sxp, axp, nx - 4, 0), (sxm, axm, 0, 3)):
        for lo in (0, 4):
            out[lo:lo + 4, MX:yend, :] = own[lo:lo + 4]
            out[lo:lo + 4, 0:MX, :] = gyl[r0:r0 + 4, lo:lo + 4, :]
            out[lo:lo + 4, yend:yend + MX, :] = gyh[r0:r0 + 4, lo:lo + 4, :]
        for t in range(3):
            row = t if line == 0 else 3 - t
            out[row, 3 - t:4 - t, :] = gyl[nx, line + t:line + t + 1, :]
            out[row, yend + t:yend + t + 1, :] = gyh[nx, line + t:line + t + 1, :]
        for h in range(2):
            for g in range(2):
                out[8 + g, h * ny:(h + 1) * ny, :] = own[8 + 2 * h + g]


def smooth_mid(b2, m2, m3, test, w3, gxl, gxh, gyl, gyh, _ryl, _ryh,
               xm, rm, kx, ky, kyp, kz, kzp, dg, w, out,
               qe, me, u, tmp):
    nx, ny, nz = b2.shape
    R = nx + 2 * MX
    shift = 4.0 * SHIFT
    xend, yend = MX + nx, MX + ny
    for ext, own, lo in ((qe, b2, 0), (me, m2, 4)):
        kept = halved if ext is me else plain
        ext[MX:xend, MX:yend, :] = kept(own[...])
        ext[MX:xend, 0:MX, :] = kept(gyl[0:nx, lo:lo + 4, :])
        ext[MX:xend, yend:yend + MX, :] = kept(gyh[0:nx, lo:lo + 4, :])
        ext[0:MX] = kept(gxl[lo:lo + 4])
        ext[xend:xend + MX] = kept(gxh[lo:lo + 4])
    co = (kx, ky, kyp, kz, kzp, dg, w)
    coefficients(me, co, R, shift, UM)
    col = lax.broadcasted_iota(jnp.int32, (ny + 2 * MX, nz), 0)
    dcol = jnp.maximum(jnp.maximum(MX - col, col - (yend - 1)), 0)

    def first(i, carry):
        di = jnp.maximum(jnp.maximum(MX - i, i - (xend - 1)), 0)
        q = qe[i]
        sent = (dcol + di == 5) | (dcol == 4) | (di == 4)
        u[i] = jnp.where(sent, q, w[i] * q)
        return carry

    u[0] = qe[0]
    u[R - 1] = qe[R - 1]
    loop(1, R - 1, first, 0, UM)

    def second(i, carry):
        au, c = apply_row(u, co, i)
        res = qe[i] - au
        rm[i] = res
        up = ALPHA * c + BETA * (w[i] * res)
        xm[i] = c + up
        qe[i] = up
        return carry

    loop(1, R - 1, second, 0, UM)

    def third(i, carry):
        au, _ = apply_row(qe, co, i)
        rm[i] = rm[i] - au
        return carry

    loop(2, R - 2, third, 0, UM)
    cx, cy = nx // 2, ny // 2
    b3 = 0.5 * add_pairs(pair_rows(rm, tmp, MX, MX, cx, cy)).reshape(cx, cy, nz // 2)
    cz = nz // 2
    kept = jnp.sum(jnp.sum(test[...] * b3, axis=0), axis=0, keepdims=True)
    mass = jnp.sum(jnp.sum(m3[...], axis=0), axis=0, keepdims=True)
    lane = lax.broadcasted_iota(jnp.int32, (1, cz), 1)
    extra = jnp.where(lane < cz // 2, kept + pltpu.roll(kept, cz // 2, 1), mass + pltpu.roll(mass, cz // 2, 1))
    lines = jnp.concatenate([(w3[...] * b3).reshape(cx * cy, cz), extra], axis=0)
    both = lines.reshape(cx * cy + 1, 1, cz)

    def put(k, carry):
        out[k] = both
        return carry

    lax.fori_loop(0, out.shape[0], put, 0, unroll=8)


def plane(f, zs):
    c1 = zs + (nxt(f, 0) + prv(f, 0))
    c2 = nxt(zs, 0) + prv(zs, 0)
    return 0.5 * c1 + 0.125 * c2, 0.5 * f + 0.125 * c1 + 0.0625 * c2


def weighted_sums(f, m, mzn, mzp, lo, hi):
    own, out = {}, {}
    for i in range(lo - 1, hi + 1):
        fn, fp = nxt(f[i], 1), prv(f[i], 1)
        a, o = plane(f[i], fn + fp)
        am, om = plane(m[i] * f[i], mzn[i] * fn + mzp[i] * fp)
        own[i], out[i] = (a, am), (o, om)
    return {i: m[i] * (own[i][0] + (out[i - 1][0] + out[i + 1][0])) + (own[i][1] + (out[i - 1][1] + out[i + 1][1]))
            for i in range(lo, hi)}


def rotate_rows(m, rows, mzn, mzp):
    for i in range(rows):
        mzn[i] = nxt(m[i], 1)
        mzp[i] = prv(m[i], 1)


def inverse_rows(m, mzn, mzp, lo, hi):
    planes = {i: plane(m[i], mzn[i] + mzp[i]) for i in range(lo - 1, hi + 1)}
    return {i: JACOBI / (16.0 * SHIFT + 0.5 * (WEIGHT_TOTAL * m[i] + (planes[i][0] + (planes[i - 1][1] + planes[i + 1][1]))))
            for i in range(lo, hi)}


def mean_weights(m9, test, w3, mzn, mzp):
    rows, (cx, cy, cz) = m9.shape[0], test.shape
    rotate_rows(m9, rows, mzn, mzp)
    w = inverse_rows(m9, mzn, mzp, 1, rows - 1)
    one = jnp.ones(m9.shape[1:], F32)
    g = {i: one for i in range(1, rows - 1)}
    total = {i: one for i in range(cx, 2 * cx)}
    for sweep in range(SWEEPS - 1):
        lo, hi = 2 + sweep, rows - 2 - sweep
        sums = weighted_sums({i: w[i] * g[i] for i in range(lo - 1, hi + 1)}, m9, mzn, mzp, lo, hi)
        g = {i: (1.0 - JACOBI) * g[i] + 0.5 * sums[i] for i in range(lo, hi)}
        total = {i: total[i] + g[i] for i in total}
    for i in range(cx):
        wi = w[cx + i]
        test[i] = (1.0 - 16.0 * SHIFT * (wi * total[cx + i]))[cy:2 * cy]
        w3[i] = wi[cy:2 * cy]


def coarse_weights(m9, gyl, gyh, gxl, gxh, mw, mzn, mzp, wc):
    rows, cz = mw.shape[0], mw.shape[2]
    mw[0] = gxl[10, :, 0:cz]
    mw[rows - 1] = gxh[10, :, 0:cz]
    for k in range(rows - 2):
        mw[1 + k] = far_lines(m9[k], k, gyl, gyh)
    rotate_rows(mw, rows, mzn, mzp)
    w = inverse_rows(mw, mzn, mzp, 1, rows - 1)
    for i in w:
        wc[i] = w[i]


def finish(got, m9, xm, rm, kx2, ky2, kyp2, kz2, kzp2, dg2, w2, x1, r1, gxl, gxh, gyl, gyh, ryl, ryh,
           kx, ky, kyp, kz, kzp, dg, w, new,
           ec, mw, mzn, mzp, wc, vm, um, t2, t3, vf, uf, qf, of, sems):
    X, Y, Z = of.shape
    nx, ny, nz = X // 2, Y // 2, Z // 2
    cx, cy, cz = nx // 2, ny // 2, nz // 2
    NX, NY = lax.axis_size("gx"), lax.axis_size("gy")
    px, py = lax.axis_index("gx"), lax.axis_index("gy")
    CY = ec.shape[1]
    rows = 3 * cx + 2
    coarse_weights(m9, gyl, gyh, gxl, gxh, mw, mzn, mzp, wc)

    for k in range(-2, 3):
        gx = lax.rem(px + k + NX, NX) * NY
        take = slice(cx - 1, cx) if k == -2 else slice(0, 1) if k == 2 else slice(0, cx)
        r0 = (k + 1) * cx + 1 if k > -2 else 0
        n = take.stop - take.start
        for l in range(-2, 3):
            slot = gx + lax.rem(py + l + NY, NY)
            for a in range(n):
                lines = got[slot, pl.ds((take.start + a) * cy, cy), 0, :]
                if l == -2:
                    ec[r0 + a, CY - 1:CY, :] = lines[cy - 1:cy]
                elif l == 2:
                    ec[r0 + a, 3 * cy:CY - 1, :] = lines[0:cy - 1]
                else:
                    ec[r0 + a, (l + 1) * cy:(l + 2) * cy, :] = lines
    e = {i: ec[i] for i in range(rows)}
    for sweep in range(SWEEPS - 1):
        lo, hi = 1 + sweep, rows - 1 - sweep
        sums = weighted_sums(e, mw, mzn, mzp, lo, hi)
        e = {i: (1.0 - JACOBI) * e[i] + (ec[i] + (0.5 * wc[i]) * sums[i]) for i in range(lo, hi)}
    sums = got[0, cx * cy]
    for k in range(1, NX * NY):
        sums = sums + got[k, cx * cy]
    cells = cx * cy * cz * NX * NY
    first = lax.broadcasted_iota(jnp.int32, (1, cz), 1) < cz // 2
    total = jnp.sum(jnp.where(first, sums, 0.0), axis=1, keepdims=True) * (1.0 / cells)
    mean_m = jnp.sum(jnp.where(first, 0.0, sums), axis=1, keepdims=True) * (1.0 / cells)
    kappa = JACOBI * total / (16.0 * SHIFT + WEIGHT_TOTAL * mean_m)

    ex, ey = cx + 4, cy + 4
    e = jnp.concatenate([e[cx - 1 + i] + kappa for i in range(ex)], axis=0)
    ed = double(e).reshape(ex, CY, nz)[:, cy - 2:cy - 2 + ey, :]
    for a in range(ex):
        both = repeat_rows(t2, ed[a])
        vm[2 * a] = both
        vm[2 * a + 1] = both
    R = nx + 2 * MX
    co2 = (kx2, ky2, kyp2, kz2, kzp2, dg2, w2)
    co = (kx, ky, kyp, kz, kzp, dg, w)

    def mid_first(i, carry):
        au, c = apply_row(vm, co2, i)
        res = rm[i] - au
        upd = w2[i] * res
        rm[i] = res
        um[i] = upd
        xm[i] = xm[i] + c + upd
        return carry

    loop(2, R - 2, mid_first, 0, UM)

    def mid_second(i, carry):
        au, c = apply_row(um, co2, i)
        xm[i] = xm[i] + (ALPHA * c + BETA * (w2[i] * (rm[i] - au)))
        return carry

    loop(3, R - 3, mid_second, 0, UM)

    wide = nx + 2
    big = double(xm[MX - 1:MX - 1 + wide].reshape(wide * (ny + 2 * MX), nz))
    big = big.reshape(wide, ny + 2 * MX, Z)[:, MX - 2:MX - 2 + ny + 4, :]
    for a in range(wide):
        both = repeat_rows(t3, big[a])
        vf[1 + 2 * a] = both
        vf[2 + 2 * a] = both
    RF = X + 2 * FX
    uf[...] = r1[...]
    for row, msg in ((FX - 1, gxl), (FX + X, gxh)):
        for g in range(2):
            uf[row, FY:FY + Y, g * nz:(g + 1) * nz] = msg[8 + g]
    for colj, msg in ((FY - 1, ryl), (FY + Y, ryh)):
        for i in range(X):
            uf[FX + i, colj:colj + 1, :] = msg[i // 8, i % 8:i % 8 + 1, :]

    def fine_first(i, carry):
        au, _ = apply_row(vf, co, i)
        res = uf[i] - au
        uf[i] = res
        qf[i] = w[i] * res
        return carry

    loop(2, RF - 2, fine_first, 0, UF)

    def fine_second(i, carry):
        au, c = apply_row(qf, co, i)
        upd = vf[i] + ((1.0 + ALPHA) * c + BETA * (w[i] * (uf[i] - au)))
        of[i - FX] = (x1[i] + upd)[FY:FY + Y]
        return carry

    part = X // PIECES
    copies = []
    for k in range(PIECES):
        lo = k * part
        loop(FX + lo, FX + lo + part, fine_second, 0, UF)
        src = of.at[pl.ds(lo, part)]
        copies.append(pltpu.make_async_copy(src, new.at[pl.ds(lo, part)], sems.at[k]))
        copies[-1].start()
    for copy in copies:
        copy.wait()


def vmem_call(body, out_shape, scratch, inputs, hbm_in=0, hbm_out=False):
    space = pl.BlockSpec(memory_space=pltpu.VMEM)
    far = pl.BlockSpec(memory_space=pltpu.HBM)
    single = not isinstance(out_shape, (list, tuple))
    return pl.pallas_call(
        body,
        out_shape=out_shape,
        in_specs=[far] * hbm_in + [space] * (len(inputs) - hbm_in),
        out_specs=(far if hbm_out else space) if single else [space] * len(out_shape),
        scratch_shapes=scratch,
        compiler_params=pltpu.CompilerParams(vmem_limit_bytes=VMEM_LIMIT),
    )(*inputs)


X_DIRS = ((1, 0), (-1, 0))
Y_DIRS = ((0, 1), (0, -1))
CORNERS = ((1, 1), (1, -1), (-1, 1), (-1, -1))


def exchange(messages, dirs):
    nx, ny = lax.axis_size("gx"), lax.axis_size("gy")
    got = []
    for msg, (dx, dy) in zip(messages, dirs):
        pairs = [(i * ny + j, ((i + dx) % nx) * ny + (j + dy) % ny) for i in range(nx) for j in range(ny)]
        got.append(lax.ppermute(msg, ("gx", "gy"), pairs))
    return got


def sd(*shape):
    return jax.ShapeDtypeStruct(shape, F32)


def vm(*shape):
    return pltpu.VMEM(shape, F32)


def local(pressure, divergence, inverse_density):
    X, Y, Z = pressure.shape
    nx, ny, nz = X // 2, Y // 2, Z // 2
    cx, cy, cz = nx // 2, ny // 2, nz // 2
    NX, NY = lax.axis_size("gx"), lax.axis_size("gy")
    xe, ye = X + 2 * FX, Y + 2 * FY
    mxe, mye = nx + 2 * MX, ny + 2 * MX
    fine = tuple(pltpu.with_memory_space_constraint(a, pltpu.HBM) for a in (pressure, divergence, inverse_density))
    msgs = vmem_call(pack_fine,
                     [sd(X, Y, Z)] * 3 + [sd(cx, cy, cz)] + [sd(X + 1, 8, Z)] * 2 + [sd(Y + 1, 8, Z)] * 2 + [sd(7 + cx, 1, Z)] * 4,
                     [vm(cx, Z // LANES, Y, LANES), pltpu.SemaphoreType.DMA((3 * PIECES,))], fine, hbm_in=3)
    got = exchange(msgs[4:], Y_DIRS + X_DIRS + CORNERS)
    res = vmem_call(
        smooth_fine,
        [sd(xe, ye, Z)] * 9 + [sd(nx, ny, nz)] * 2
        + [sd(3 * cx, 4 * cy, cz)] + [sd(12, ny, nz)] * 2 + [sd(nx + 2, 8, nz)] * 2 + [sd(X // 8, 8, Z)] * 2,
        [vm(xe, ye, Z)] * 3 + [vm(nx, Z // LANES, ye, LANES), vm(nx + 2, Z // LANES, ye, LANES)],
        tuple(msgs[:4]) + tuple(got))
    x1, r1 = res[:2]
    fine_co = tuple(res[2:9])
    b2, m2, m9 = res[9:12]
    m3 = msgs[3]
    test, w3 = vmem_call(mean_weights, [sd(cx, cy, cz)] * 2, [vm(3 * cx, 4 * cy, cz)] * 2, (m9,))
    cols = exchange(res[14:16], Y_DIRS)
    edges = exchange(res[16:18], Y_DIRS)
    spread = vmem_call(spread_rows, [sd(11, mye, nz)] * 2, [], (*cols, *res[12:14], m9))
    rows = exchange(spread, X_DIRS)
    got2 = rows + cols
    *mid, out = vmem_call(
        smooth_mid,
        [sd(mxe, mye, nz)] * 9 + [sd(NX * NY, cx * cy + 1, 1, cz)],
        [vm(mxe, mye, nz)] * 3 + [vm(cx, nz // LANES, mye, LANES)],
        (b2, m2, m3, test, w3) + tuple(got2) + tuple(edges))
    gathered = lax.all_to_all(out, ("gx", "gy"), 0, 0)
    window = (3 * cx + 2, 4 * cy, cz)
    return vmem_call(
        finish, sd(X, Y, Z),
        [vm(*window)] * 5 + [vm(mxe, mye, nz)] * 2 + [vm(nz // LANES, mye, LANES), vm(Z // LANES, ye, LANES)]
        + [vm(xe, ye, Z)] * 3 + [vm(X, Y, Z), pltpu.SemaphoreType.DMA((PIECES,))],
        (gathered, m9, *mid, x1, r1) + tuple(got2) + tuple(edges) + fine_co, hbm_out=True)


def solution(mesh):
    return jax.shard_map(
        local,
        mesh=mesh,
        in_specs=(P("gx", "gy", None),) * 3,
        out_specs=P("gx", "gy", None),
        check_vma=False,
    )
```
